32 devices in a mesh: row: 4 (over z), col: 8 (over y, x, core).
Axes of the slice: x: 2, y: 2, z: 4, core: 2. Of those that a mesh axis runs over, the one named last changes fastest.
Arguments:
- clean: float32 [1344, 8192], P('row', 'col'), may hold values from -6 to 6
- noise: float32 [1344, 8192], P('row', 'col'), may hold values from -6 to 6
- bucket: int32 [32], replicated, may hold values from 0 to 31
- mod_table: float32 [1, 32, 1344], replicated, may hold values from -3 to 3
- w_first: float32 [1, 1344, 1344], P(None, 'row', 'col'), may hold values from -0.15625 to 0.15625
- w_second: float32 [1, 1344, 1344], P(None, 'col', 'row'), may hold values from -0.15625 to 0.15625
Outputs:
- grad_first: float32 [1, 1344, 1344], P(None, 'row', 'col')
- grad_second: float32 [1, 1344, 1344], P(None, 'col', 'row')
The draws below stay inside these ranges and needn't reach their ends.
All inputs are finite; a program needn't handle non-finite values.
Results may differ from the reference program's by a relative error of at most 0.018.
Values may be sent and summed in bfloat16 or wider, within the bound.
A program may use at most 64 MiB of HBM per device.

```python
import math
import jax
import jax.numpy as jnp
from jax import lax

WIDTH = 1344
PIX = 256
BLOCKS = 1
BUCKETS = 32
SAMPLES = 32


def place_ends(array, own_key, least, top_value):
    longest = array.shape.index(max(array.shape))
    spots = []
    for shift in (0, 1):
        where = [jax.random.randint(jax.random.fold_in(own_key, axis), (), 0, length) for axis, length in enumerate(array.shape)]
        where[longest] = (where[longest] + shift) % array.shape[longest]
        spots.append(tuple(where))
    return array.at[spots[0]].set(least).at[spots[1]].set(top_value)


def shard_levels(rng, extent, cuts, low, high):
    def one(dim, shards_of):
        heights = jax.random.uniform(jax.random.fold_in(jax.random.fold_in(rng, 6), dim), (shards_of,), jnp.float32, low / len(cuts), high / len(cuts))
        return jnp.repeat(jnp.exp(heights), extent[dim] // shards_of).reshape((-1,) + (1,) * (len(extent) - dim - 1))

    level = one(*cuts[0])
    for cut in cuts[1:]:
        level = level * one(*cut)
    return level


def scatter_about(stream_key, dims, deviation, bound, cuts=(), kind=jnp.bfloat16):
    values = jax.random.normal(stream_key, dims, jnp.float32) * deviation
    if len(cuts) > 0:
        values = shard_levels(stream_key, dims, cuts, -0.22, 0.18) * values
    return jnp.clip(values, min=-bound, max=bound).astype(kind)


def setup_inputs(seed: int = 0) -> dict:
    seeds = jax.random.split(jax.random.key(seed), 7)
    clean = scatter_about(seeds[0], (WIDTH, SAMPLES * PIX), 1.0, 6.0, ((0, 4), (1, 8)), jnp.float32)
    noise = scatter_about(seeds[1], (WIDTH, SAMPLES * PIX), 1.0, 6.0, ((0, 4), (1, 8)), jnp.float32)
    bucket = place_ends(jax.random.randint(seeds[2], (SAMPLES,), 0, BUCKETS), jax.random.fold_in(seeds[2], 1), 0, BUCKETS - 1).astype(jnp.int32)
    mod_table = scatter_about(seeds[3], (BLOCKS, BUCKETS, WIDTH), 0.3, 3.0, (), jnp.float32)
    w_first = scatter_about(seeds[4], (BLOCKS, WIDTH, WIDTH), WIDTH ** -0.5, 0.15625, ((1, 4), (2, 8)), jnp.float32)
    w_second = scatter_about(seeds[5], (BLOCKS, WIDTH, WIDTH), WIDTH ** -0.5, 0.15625, ((1, 8), (2, 4)), jnp.float32)
    return dict(clean=clean, noise=noise, bucket=bucket, mod_table=mod_table, w_first=w_first, w_second=w_second)


MIX_WEIGHT = 0.3
KEEP_COEF = (1.0 - MIX_WEIGHT) / math.sqrt((1.0 - MIX_WEIGHT) ** 2 + MIX_WEIGHT ** 2)
ADD_COEF = MIX_WEIGHT / math.sqrt((1.0 - MIX_WEIGHT) ** 2 + MIX_WEIGHT ** 2)
SILU_GAIN = 1.0 / 0.596

def noise_levels(bucket):
    return jnp.exp(-3.0 + 5.0 * (bucket.astype(jnp.float32) + 0.5) / BUCKETS)

def silu_slope(values):
    sig = jax.nn.sigmoid(values)
    return sig * (1.0 + values * (1.0 - sig))

def reference(clean, noise, bucket, mod_table, w_first, w_second):
    clean = clean.T
    noise = noise.T
    levels = jnp.repeat(noise_levels(bucket), PIX)[:, None]
    spread_root = jnp.sqrt(levels * levels + 0.25)
    state = ((clean + levels * noise) / spread_root).astype(jnp.bfloat16)
    target = clean * (2.0 * levels / spread_root) - noise * (0.5 / spread_root)
    onehot = (bucket[:, None] == jnp.arange(BUCKETS, dtype=jnp.int32)[None, :]).astype(jnp.float32)
    saved = []
    for block in range(BLOCKS):
        col_first = jnp.sqrt(lax.optimization_barrier(jnp.sum(w_first[block] * w_first[block], axis=0)) + 1.0)
        col_second = jnp.sqrt(lax.optimization_barrier(jnp.sum(w_second[block] * w_second[block], axis=0)) + 1.0)
        normed_first = (w_first[block] / col_first[None, :]).astype(jnp.bfloat16)
        normed_second = (w_second[block] / col_second[None, :]).astype(jnp.bfloat16)
        gains = jnp.dot(onehot, 1.0 + mod_table[block], precision=lax.Precision.HIGHEST, preferred_element_type=jnp.float32)
        gains = jnp.repeat(gains, PIX, axis=0)
        pre_act = jnp.dot(state, normed_first, preferred_element_type=jnp.float32)
        hidden = (jax.nn.silu(pre_act) * SILU_GAIN * gains).astype(jnp.bfloat16)
        branch = jnp.dot(hidden, normed_second, preferred_element_type=jnp.float32)
        saved.append((state, hidden, pre_act, gains, normed_first, normed_second, col_first, col_second))
        state = (KEEP_COEF * state.astype(jnp.float32) + ADD_COEF * branch).astype(jnp.bfloat16)
    grad_state = (state.astype(jnp.float32) - target) / SAMPLES
    firsts = []
    seconds = []
    for block in range(BLOCKS - 1, -1, -1):
        state_in, hidden, pre_act, gains, normed_first, normed_second, col_first, col_second = saved[block]
        dbranch = (ADD_COEF * grad_state).astype(jnp.bfloat16)
        gsecond = jnp.dot(hidden.T, dbranch, preferred_element_type=jnp.float32)
        dhidden = jnp.dot(dbranch, normed_second.T, preferred_element_type=jnp.float32)
        dpre = (dhidden * gains * silu_slope(pre_act) * SILU_GAIN).astype(jnp.bfloat16)
        gfirst = jnp.dot(state_in.T, dpre, preferred_element_type=jnp.float32)
        if block > 0:
            grad_state = KEEP_COEF * grad_state + jnp.dot(dpre, normed_first.T, preferred_element_type=jnp.float32)
        dot_first = lax.optimization_barrier(jnp.sum(w_first[block] * gfirst, axis=0))
        dot_second = lax.optimization_barrier(jnp.sum(w_second[block] * gsecond, axis=0))
        firsts.append(gfirst / col_first[None, :] - w_first[block] * (dot_first / col_first ** 3)[None, :])
        seconds.append(gsecond / col_second[None, :] - w_second[block] * (dot_second / col_second ** 3)[None, :])
    grad_first = jnp.stack(firsts[::-1], axis=0)
    grad_second = jnp.stack(seconds[::-1], axis=0)
    return (grad_first, grad_second)
```

```python
import math

import jax
import jax.numpy as jnp
from jax import lax
from jax.experimental import pallas as pl
from jax.experimental.pallas import tpu as pltpu
from jax.sharding import PartitionSpec as P

PIX = 256
BUCKETS = 32


MIX_WEIGHT = 0.3
KEEP_COEF = (1.0 - MIX_WEIGHT) / math.sqrt((1.0 - MIX_WEIGHT) ** 2 + MIX_WEIGHT**2)
ADD_COEF = MIX_WEIGHT / math.sqrt((1.0 - MIX_WEIGHT) ** 2 + MIX_WEIGHT**2)
SILU_GAIN = 1.0 / 0.596
CONTRACT_LEAD = (((0,), (0,)), ((), ()))
CONTRACT_TAIL = (((1,), (1,)), ((), ()))


def noise_levels(bucket):
    return jnp.exp(-3.0 + 5.0 * (bucket.astype(jnp.float32) + 0.5) / BUCKETS)


def silu_slope(values):
    sig = jax.nn.sigmoid(values)
    return sig * (1.0 + values * (1.0 - sig))


def bucket_gains(table, picked):
    onehot = (picked[:, None] == jnp.arange(table.shape[0], dtype=jnp.int32)[None, :]).astype(
        jnp.float32
    )
    return jnp.dot(
        onehot, table, precision=lax.Precision.HIGHEST, preferred_element_type=jnp.float32
    )


def local(clean, noise, bucket, mod_table, w_first, w_second):
    rows_size = lax.axis_size("row")
    row_at = lax.axis_index("row")
    col_at = lax.axis_index("col")
    samples = bucket.shape[0]
    own_rows = clean.shape[1]
    weight_first = w_first[0]
    weight_second = w_second[0]
    table = 1.0 + mod_table[0]
    col_first = jnp.sqrt(lax.psum(jnp.sum(weight_first * weight_first, axis=0), "row") + 1.0)
    col_second = jnp.sqrt(lax.psum(jnp.sum(weight_second * weight_second, axis=0), "col") + 1.0)
    normed_first = (weight_first / col_first[None, :]).astype(jnp.bfloat16)
    normed_second = (weight_second / col_second[None, :]).astype(jnp.bfloat16)
    chan_clean, chan_noise = (
        lax.all_to_all(
            clean.astype(jnp.bfloat16), "row", split_axis=1, concat_axis=0, tiled=True
        ).astype(clean.dtype),
        lax.all_to_all(
            noise.astype(jnp.bfloat16), "row", split_axis=1, concat_axis=0, tiled=True
        ).astype(noise.dtype),
    )
    local_clean = chan_clean.T
    local_noise = chan_noise.T
    sub_rows = own_rows // rows_size
    first_row = col_at * own_rows + row_at * sub_rows
    row_sample = (first_row + jnp.arange(sub_rows, dtype=jnp.int32)) // PIX
    row_bucket = jnp.take(bucket, row_sample)
    levels = noise_levels(row_bucket)[:, None]
    spread_root = jnp.sqrt(levels * levels + 0.25)
    state_own = ((local_clean + levels * local_noise) / spread_root).astype(jnp.bfloat16)
    target = local_clean * (2.0 * levels / spread_root) - local_noise * (0.5 / spread_root)
    gains = bucket_gains(table, row_bucket)
    part_first, part_second = (
        lax.all_gather(normed_first, "col", axis=1, tiled=True),
        lax.all_gather(normed_second, "col", axis=0, tiled=True),
    )
    full_first, full_second = (
        lax.all_gather(part_first, "row", axis=0, tiled=True),
        lax.all_gather(part_second, "row", axis=1, tiled=True),
    )
    pre_act = jnp.dot(state_own, full_first, preferred_element_type=jnp.float32)
    hidden = (jax.nn.silu(pre_act) * SILU_GAIN * gains).astype(jnp.bfloat16)
    branch = jnp.dot(hidden, full_second, preferred_element_type=jnp.float32)
    state_new = (KEEP_COEF * state_own.astype(jnp.float32) + ADD_COEF * branch).astype(jnp.bfloat16)
    grad_own = (state_new.astype(jnp.float32) - target) / samples
    dbranch = (ADD_COEF * grad_own).astype(jnp.bfloat16)
    gsecond_full = lax.dot_general(
        hidden, dbranch, CONTRACT_LEAD, preferred_element_type=jnp.float32
    )
    dhidden = lax.dot_general(
        dbranch, full_second, CONTRACT_TAIL, preferred_element_type=jnp.float32
    )
    dpre = (dhidden * gains * silu_slope(pre_act) * SILU_GAIN).astype(jnp.bfloat16)
    gfirst_full = lax.dot_general(
        state_own, dpre, CONTRACT_LEAD, preferred_element_type=jnp.float32
    )
    part_gfirst, part_gsecond = (
        lax.psum_scatter(
            gfirst_full.astype(jnp.bfloat16), "col", scatter_dimension=1, tiled=True
        ).astype(jnp.float32),
        lax.psum_scatter(
            gsecond_full.astype(jnp.bfloat16), "col", scatter_dimension=0, tiled=True
        ).astype(jnp.float32),
    )
    gfirst, gsecond = (
        lax.psum_scatter(
            part_gfirst.astype(jnp.bfloat16), "row", scatter_dimension=0, tiled=True
        ).astype(jnp.float32),
        lax.psum_scatter(
            part_gsecond.astype(jnp.bfloat16), "row", scatter_dimension=1, tiled=True
        ).astype(jnp.float32),
    )
    dot_first = lax.psum(jnp.sum(weight_first * gfirst, axis=0), "row")
    dot_second = lax.psum(jnp.sum(weight_second * gsecond, axis=0), "col")
    grad_first = gfirst / col_first[None, :] - weight_first * (dot_first / col_first**3)[None, :]
    grad_second = (
        gsecond / col_second[None, :] - weight_second * (dot_second / col_second**3)[None, :]
    )
    return (grad_first[None], grad_second[None])


CORES = 2
SIDE = 2
MESH = pl.DeviceIdType.MESH


def round_up(size, unit):
    return -(-size // unit) * unit


def twice(value):
    return jnp.concatenate([value, value], axis=1)


def split_sum(total):
    high = total.astype(jnp.bfloat16)
    low = (total - high.astype(jnp.float32)).astype(jnp.bfloat16)
    return high, low


def step_kernel(
    hb, ib, samples, names, bucket, clean, noise, table, w1h, w2h, out1, out2,
    cl, no, w1f, w2f, sto, w, st, tg, nrm, gain, pre, slp, hid, brk, brp, brr, dbr, db2, dpre,
    s2, d2, dot1, g, ra, sa, rb, rc, pz, rz, sems, local_sems,
):
    rows = st.shape[0] // round_up(ib + 1, 128)
    hp, ip = round_up(hb + 2, 16), round_up(ib + 1, 128)
    chips = w.shape[1] // hp
    sub = tg.shape[1]
    hh, ii = chips * hp, rows * ip
    own_rows = cl.shape[1]
    bf16, f32 = jnp.bfloat16, jnp.float32
    z = lax.axis_index("row")
    col = lax.axis_index("col")
    core = lax.rem(col, CORES)
    xy = col // CORES
    x, y = lax.rem(xy, SIDE), xy // SIDE
    xn = y * SIDE + (1 - x)
    yn = (1 - y) * SIDE + x
    dn = (1 - y) * SIDE + (1 - x)
    dev_x = (z, xn * CORES + core)
    dev_y = (z, yn * CORES + core)
    dev_p = (z, xy * CORES + 1 - core)
    up, down = (z + 1, col), (z - 1, col)
    ring = [lax.rem(z + k, rows) for k in range(rows)]
    side = 1 - 2 * (z // (rows // 2))
    near = [z] + [lax.rem(z + side * k + rows, rows) for k in range(1, rows)]

    loads = []
    for k, (src, dst) in enumerate([(w1h, w1f), (w2h, w2f), (clean, cl), (noise, no)]):
        loads.append(pltpu.make_async_copy(src, dst, local_sems.at[k]))
        loads[-1].start()
    barrier = pltpu.get_barrier_semaphore()
    peers = [dev_x, dev_y, dev_p] + [(ring[k], col) for k in range(1, rows)]
    for peer in peers:
        pl.semaphore_signal(barrier, inc=1, device_id=peer, device_id_type=MESH)

    pending = []

    def sem(kind, at):
        return sems.at[names.setdefault(kind, len(names)), at]

    def remote(src, dst, kind, at_send, at_recv, dev):
        return pltpu.make_async_remote_copy(
            src_ref=src, dst_ref=dst, send_sem=sem("s" + kind, at_send),
            recv_sem=sem("r" + kind[:2], at_recv), device_id=dev, device_id_type=MESH,
        )

    def when(cond, fn):
        if cond is None:
            fn()
        else:
            pl.when(cond)(fn)

    def send(cond, *spec):
        when(cond, lambda: remote(*spec).start())
        pending.append((cond, spec))

    def arrive(cond, dst, kind, at):
        flag = sem("r" + kind, at)
        when(cond, lambda: pltpu.make_async_remote_copy(
            src_ref=dst, dst_ref=dst, send_sem=flag, recv_sem=flag, device_id=dev_p, device_id_type=MESH,
        ).wait_recv())

    def span(start, size, unit):
        return pl.ds(pl.multiple_of(start, unit), size)

    def cut(m):
        return round_up(hp // 2, 16) if m == 0 else hp - round_up(hp // 2, 16)

    def part_rows(m, p):
        return (0, cut(m)) if p == 0 else (cut(m), hp - cut(m))

    def wblk(m, xyb, zb, p=None):
        lo, size = (0, hp) if p is None else part_rows(m, p)
        return w.at[m, span(xyb * hp + lo, size, 16), span(zb * ip, ip, 128)]

    def chan(zb, size=ib):
        return span(zb * ip, size, 16)

    def pix(zb):
        return span(zb * sub, sub, 128)

    mine, other = slice(0, sub), slice(sub, 2 * sub)

    for zb in range(rows):
        pad = slice(zb * ip + ib, (zb + 1) * ip)
        st[pad, :] = jnp.zeros((ip - ib, 2 * sub), bf16)
        tg[pad, :] = jnp.zeros((ip - ib, sub), bf16)

    line = lax.broadcasted_iota(jnp.int32, (hp, ip), 0)
    for m, full in enumerate((w1f, w2f)):
        loads[m].wait()
        block = jnp.pad(full[...], ((0, hp - hb), (0, ip - ib)))
        if m == 0:
            total = jnp.sum(block * block, axis=1, keepdims=True)
            total = jnp.pad(jnp.broadcast_to(total, (hp, 128)), ((0, 256 - hp), (0, 0)))
            total = jnp.pad(total.T[:1, :], ((0, 0), (0, ip - 256)))
        else:
            total = jnp.sum(block * block, axis=0, keepdims=True)
        high, low = split_sum(total)
        block = jnp.where(line == hb, high.astype(f32), block)
        block = jnp.where(line == hb + 1, low.astype(f32), block)
        w[m, span(xy * hp, hp, 16), span(z * ip, ip, 128)] = block.astype(bf16)
    pl.semaphore_wait(barrier, len(peers))

    def along_z(cond, m, zb, go_up, go_down):
        if go_up:
            send(both(cond, z + 1 < rows), wblk(m, xy, zb), wblk(m, xy, zb), f"z{m}u", zb, zb, up)
        if go_down:
            send(both(cond, z > 0), wblk(m, xy, zb), wblk(m, xy, zb), f"z{m}d", zb, zb, down)

    def both(a, b):
        return b if a is None else jnp.logical_and(a, b)

    def across(cond, m, zb):
        send(cond, wblk(m, xy, zb), wblk(m, xy, zb), f"x{m}", zb, zb, dev_x)
        send(cond, wblk(m, xy, zb), wblk(m, xy, zb), f"y{m}", zb, zb, dev_y)

    def diagonal(cond, m, zb):
        arrive(cond, wblk(m, xn, zb), f"x{m}", zb)
        send(cond, wblk(m, xn, zb, 0), wblk(m, xn, zb, 0), f"a{m}", zb, zb, dev_y)
        arrive(cond, wblk(m, yn, zb), f"y{m}", zb)
        send(cond, wblk(m, yn, zb, 1), wblk(m, yn, zb, 1), f"b{m}", zb, zb, dev_x)

    def sides(d):
        return ((z - d >= 0, z - d, True, False), (z + d < rows, z + d, False, True))

    def hop(m, d):
        for cond, zb, go_up, go_down in sides(d):
            arrive(cond, wblk(m, xy, zb), f"z{m}", zb)
            along_z(cond, m, zb, go_up and d < rows - 1, go_down and d < rows - 1)

    def each_side(fn, m, d):
        if d == 0:
            fn(None, m, z)
        else:
            for cond, zb, _, _ in sides(d):
                fn(cond, m, zb)

    for m in range(2):
        along_z(None, m, z, True, True)
    for m in range(2):
        across(None, m, z)

    loads[2].wait()
    loads[3].wait()
    for k in range(rows):
        lanes = slice(k * sub, (k + 1) * sub)
        picked = jnp.full((1, sub), bucket[col * rows + k], jnp.int32)
        level = noise_levels(picked)
        root = jnp.sqrt(level * level + 0.25)
        c, n = cl[:, lanes], no[:, lanes]
        sto[0, :, lanes] = ((c + level * n) / root).astype(bf16)
        sto[1, :, lanes] = (c * (2.0 * level / root) - n * (0.5 / root)).astype(bf16)
    st[chan(z), mine] = sto[0, :, pix(z)]
    tg[chan(z), :] = sto[1, :, pix(z)]

    def state_to_partner(zb):
        send(None, st.at[chan(zb), mine], st.at[chan(zb), other], "f", zb, zb, dev_p)

    hop(0, 1)
    each_side(across, 0, 1)
    each_side(diagonal, 0, 0)
    hop(1, 1)
    for k in range(1, rows):
        send(None, sto.at[0, :, pix(ring[k])], st.at[chan(z), mine], "t", k, z, (ring[k], col))
    state_to_partner(z)
    each_side(diagonal, 1, 0)
    if rows > 2:
        hop(0, 2)
        each_side(across, 0, 2)
    each_side(across, 1, 1)
    each_side(diagonal, 0, 1)
    if rows > 2:
        hop(1, 2)
    for k in range(1, rows):
        zt = near[k]
        send(None, sto.at[1, :, pix(zt)], tg.at[chan(z), :], "g", k, z, (zt, col))
    for d in range(3, rows):
        hop(0, d)
        each_side(across, 0, d)
    if rows > 2:
        each_side(diagonal, 0, 2)
    each_side(diagonal, 1, 1)
    for d in range(3, rows):
        hop(1, d)
    for d in range(2, rows):
        each_side(across, 1, d)
    stack = []
    for j in range(CORES):
        whose = core if j == 0 else 1 - core
        picked = bucket[(xy * CORES + whose) * rows + z]
        row = 1.0 + table[pl.ds(picked, 1), :]
        for b in range(chips):
            pieces = [row[:, (b * CORES + c) * hb : (b * CORES + c + 1) * hb] for c in range(CORES)]
            piece = jnp.where(core == 0, pieces[0], pieces[1])
            stack.append(jnp.pad(piece, ((0, 0), (0, 256 - hb))))
    for k in range(1, rows):
        zb = ring[rows - k]
        arrive(None, st.at[chan(zb), mine], "t", zb)
        state_to_partner(zb)
    for d in range(3, rows):
        each_side(diagonal, 0, d)
    for zb in range(rows):
        arrive(None, wblk(0, dn, zb, 0), "a0", zb)
        arrive(None, wblk(0, dn, zb, 1), "b0", zb)

    def sums_of(m, b, lanes):
        tail = w[m, (b + 1) * hp - 16 : (b + 1) * hp, lanes].astype(f32)
        at = hb - (hp - 16)
        return tail[at : at + 1, :] + tail[at + 1 : at + 2, :]

    for b in range(chips):
        stack.append(sum(sums_of(0, b, slice(zb * ip, zb * ip + 256)) for zb in range(rows)))
    filler = 128 - len(stack)
    columns = jnp.concatenate(stack + [jnp.zeros((filler, 256), f32)], axis=0).T
    for b in range(chips):
        at = slice(b * hp, (b + 1) * hp)
        for j in range(CORES):
            k = j * chips + b
            gain[j, at, :] = jnp.broadcast_to(columns[:hp, k : k + 1], (hp, 128))
        k = CORES * chips + b
        nrm[at, :] = jnp.broadcast_to(jnp.sqrt(1.0 + columns[:hp, k : k + 1]), (hp, 128))
    for zb in range(rows):
        arrive(None, st.at[chan(zb), other], "f", zb)

    half_rows = hh // 2

    def forward(part):
        at = slice(part * half_rows, (part + 1) * half_rows)
        value = jnp.dot(w[0, at, :], st[...], preferred_element_type=f32)
        inverse = twice(1.0 / nrm[at, :])
        for j in range(CORES):
            lanes = slice(j * sub, (j + 1) * sub)
            v = value[:, lanes] * inverse
            sig = jax.nn.sigmoid(v)
            scale = twice(gain[j, at, :]) * SILU_GAIN
            pre[at, lanes] = v
            hid[at, lanes] = (v * sig * scale).astype(bf16)
            slp[at, lanes] = sig * (1.0 + v * (1.0 - sig)) * scale

    forward(0)
    if rows > 2:
        each_side(diagonal, 1, 2)
    forward(1)
    for d in range(3, rows):
        each_side(diagonal, 1, d)

    def zlanes(zb):
        return span(zb * ip, ip, 128)

    def branch_part(i):
        zb = near[i]
        at = zlanes(zb)
        arrive(None, wblk(1, dn, zb, 0), "a1", zb)
        arrive(None, wblk(1, dn, zb, 1), "b1", zb)
        total = sum(sums_of(1, b, at) for b in range(chips))
        s2[0, :, at] = jnp.broadcast_to(total, (s2.shape[1], ip))
        send(None, s2.at[0, :, at], s2.at[1, :, at], "n", i, zb, dev_p)
        full = lax.dot_general(w[1, :, at], hid[...], CONTRACT_LEAD, preferred_element_type=f32)
        brp[at, :] = full[:, other]
        send(None, brp.at[at, :], brr.at[at, :], "p", i, zb, dev_p)
        brk[at, :] = full[:, mine]

    def slope_part(i):
        zb = near[i]
        at = zlanes(zb)
        if i > 0:
            arrive(None, tg.at[chan(zb), :], "g", zb)
        arrive(None, s2.at[1, :, at], "n", zb)
        total = 1.0 + s2[0, :1, at] + s2[1, :1, at]
        norm = jnp.sqrt(jnp.broadcast_to(total, (128, ip)).T)
        inverse = 1.0 / norm
        arrive(None, brr.at[at, :], "p", zb)
        branch = (brk[at, :] + brr[at, :]) * twice(inverse)
        fresh = (KEEP_COEF * st[at, mine].astype(f32) + ADD_COEF * branch).astype(bf16)
        slope = (fresh.astype(f32) - tg[at, :].astype(f32)) / samples
        rounded = (ADD_COEF * slope).astype(bf16)
        dbr[at, mine] = rounded
        send(None, dbr.at[at, mine], dbr.at[at, other], "q", i, zb, dev_p)
        wide_rounded = rounded.astype(f32)
        db2[at, mine] = (wide_rounded * twice(inverse)).astype(bf16)
        product = jnp.sum(branch * wide_rounded, axis=1, keepdims=True) * norm
        d2[0, :, at] = product.T[: d2.shape[1], :]
        send(None, d2.at[0, :, at], d2.at[1, :, at], "d", i, zb, dev_p)

    hidden_line = lax.broadcasted_iota(jnp.int32, (hp, 1), 0)

    def second_part(i):
        zb = near[i]
        at = zlanes(zb)
        arrive(None, dbr.at[at, other], "q", zb)
        arrive(None, d2.at[1, :, at], "d", zb)
        second = lax.dot_general(hid[...], dbr[at, :], CONTRACT_TAIL, preferred_element_type=f32)
        dot2 = d2[0, :1, at] + d2[1, :1, at]
        for b in range(chips):
            part = second[b * hp : (b + 1) * hp, :]
            g[1, b * hp : (b + 1) * hp, at] = jnp.where(hidden_line >= hb, dot2, part).astype(bf16)
        total = jnp.broadcast_to(1.0 + s2[0, :1, at] + s2[1, :1, at], (128, ip))
        inverse = 1.0 / jnp.sqrt(total.T)
        db2[at, other] = (dbr[at, other].astype(f32) * twice(inverse)).astype(bf16)

    def backward():
        for part in range(2):
            at = slice(part * half_rows, (part + 1) * half_rows)
            grad = jnp.dot(w[1, at, :], db2[...], preferred_element_type=f32)
            rounded = (grad * slp[at, :]).astype(bf16)
            dpre[at, :] = rounded
            total = jnp.sum(rounded.astype(f32) * pre[at, :], axis=1, keepdims=True)
            dot1[at, :] = total * nrm[at, :]

    lane = lax.broadcasted_iota(jnp.int32, (1, ip), 1)
    last = [ring[k] for k in range(1, rows)] + [z]
    orders = (last, near)

    def first_part(i):
        zb = last[i]
        at = zlanes(zb)
        first = lax.dot_general(dpre[...], st[at, :], CONTRACT_TAIL, preferred_element_type=f32)
        g[0, :, at] = jnp.where(lane >= ib, dot1[:, :1], first).astype(bf16)

    def gblk(m, xyb, zb, p):
        lo, size = part_rows(m, p)
        return (m, span(xyb * hp + lo, size, 16), span(zb * ip, ip, 128))

    def rblk(ref, m, i, p):
        lo, size = part_rows(m, p)
        return ref.at[m, i, slice(lo, lo + size), :]

    def legs(p):
        return (yn, dev_y, xn, dev_x) if p == 0 else (xn, dev_x, yn, dev_y)

    def stage_a(m, i):
        zb = orders[m][i]
        for p in range(2):
            nb1, dev1, nb2, dev2 = legs(p)
            send(None, g.at[gblk(m, dn, zb, p)], rblk(ra, m, i, p), f"{'AB'[p]}{m}", i, i, dev1)
        for p in range(2):
            nb1, dev1, nb2, dev2 = legs(p)
            send(None, g.at[gblk(m, nb1, zb, p)], rblk(rc, m, i, p), f"{'CD'[p]}{m}", i, i, dev1)

    def stage_b(m, i):
        zb = orders[m][i]
        for p in range(2):
            nb1, dev1, nb2, dev2 = legs(p)
            arrive(None, rblk(ra, m, i, p), f"{'AB'[p]}{m}", i)
            lo, size = part_rows(m, p)
            inside = (m, i, slice(lo, lo + size))
            sa[inside] = (g[gblk(m, nb2, zb, p)].astype(f32) + ra[inside].astype(f32)).astype(bf16)
            send(None, rblk(sa, m, i, p), rblk(rb, m, i, p), f"{'EF'[p]}{m}", i, i, dev2)

    def stage_c(m, i):
        zb = orders[m][i]
        for p in range(2):
            arrive(None, rblk(rc, m, i, p), f"{'CD'[p]}{m}", i)
            arrive(None, rblk(rb, m, i, p), f"{'EF'[p]}{m}", i)
        own = g[m, span(xy * hp, hp, 16), span(zb * ip, ip, 128)].astype(f32)
        total = own + rb[m, i].astype(f32) + rc[m, i].astype(f32)
        own_at = rows - 1 if m == 0 else 0
        if i == own_at:
            return total
        pz[m, i] = total.astype(bf16)
        send(None, pz.at[m, i], rz.at[m, z], f"P{m}", i, z, (zb, col))
        return None

    sums = [None, None]
    branch_part(0)
    branch_part(1)
    slope_part(0)
    branch_part(2)
    slope_part(1)
    second_part(0)
    stage_a(1, 0)
    branch_part(3)
    second_part(1)
    stage_a(1, 1)
    stage_b(1, 0)
    slope_part(2)
    second_part(2)
    stage_a(1, 2)
    stage_b(1, 1)
    slope_part(3)
    second_part(3)
    stage_a(1, 3)
    sums[1] = stage_c(1, 0)
    stage_b(1, 2)
    backward()
    stage_b(1, 3)
    first_part(0)
    stage_a(0, 0)
    stage_c(1, 1)
    first_part(1)
    stage_a(0, 1)
    stage_c(1, 2)
    stage_b(0, 0)
    first_part(2)
    stage_a(0, 2)
    stage_c(1, 3)
    stage_b(0, 1)
    first_part(3)
    stage_a(0, 3)
    stage_c(0, 0)
    stage_b(0, 2)
    stage_c(0, 1)
    stage_b(0, 3)
    for k in range(1, rows):
        arrive(None, rz.at[1, ring[k]], "P1", ring[k])
    second = sums[1]
    norm2 = jnp.sqrt(1.0 + s2[0, :1, zlanes(z)] + s2[1, :1, zlanes(z)])[:, :ib]
    for k in range(1, rows):
        second = second + rz[1, ring[k]].astype(f32)
    dot_second = second[hb : hb + 1, :ib]
    out2[...] = second[:hb, :ib] / norm2 - w2f[...] * (dot_second / (norm2 * norm2 * norm2))
    stage_c(0, 2)
    first = stage_c(0, 3)
    for k in range(1, rows):
        arrive(None, rz.at[0, ring[k]], "P0", ring[k])
        first = first + rz[0, ring[k]].astype(f32)
    norm1 = nrm[span(xy * hp, hp, 16), :1][:hb]
    dot_first = first[:hb, ib : ib + 1]
    out1[...] = first[:hb, :ib] / norm1 - w1f[...] * (dot_first / (norm1 * norm1 * norm1))
    for cond, spec in pending:
        when(cond, lambda spec=spec: remote(*spec).wait_send())
    assert len(names) <= sems.shape[0], len(names)


def local_step(clean, noise, bucket, mod_table, w_first, w_second):
    rows = lax.axis_size("row")
    cols = lax.axis_size("col")
    samples = bucket.shape[0]
    own_rows = clean.shape[1]
    ib, hb = clean.shape[0], w_first.shape[2]
    sub = own_rows // rows
    if sub != PIX or rows != 4:
        return local(clean, noise, bucket, mod_table, w_first, w_second)
    chips = cols // CORES
    hp, ip = round_up(hb + 2, 16), round_up(ib + 1, 128)
    bf16, f32 = jnp.bfloat16, jnp.float32
    hh, ii = chips * hp, rows * ip
    vmem = pl.BlockSpec(memory_space=pltpu.VMEM)
    smem = pl.BlockSpec(memory_space=pltpu.SMEM)
    anywhere = pl.BlockSpec(memory_space=pl.ANY)
    out1, out2 = pl.pallas_call(
        lambda *refs: step_kernel(hb, ib, samples, {}, *refs),
        out_shape=(jax.ShapeDtypeStruct((hb, ib), f32), jax.ShapeDtypeStruct((hb, ib), f32)),
        in_specs=[smem, anywhere, anywhere, vmem, anywhere, anywhere],
        out_specs=(vmem, vmem),
        scratch_shapes=[
            pltpu.VMEM((ib, own_rows), f32),
            pltpu.VMEM((ib, own_rows), f32),
            pltpu.VMEM((hb, ib), f32),
            pltpu.VMEM((hb, ib), f32),
            pltpu.VMEM((2, ib, own_rows), bf16),
            pltpu.VMEM((2, hh, ii), bf16),
            pltpu.VMEM((ii, CORES * sub), bf16),
            pltpu.VMEM((ii, sub), bf16),
            pltpu.VMEM((hh, 128), f32),
            pltpu.VMEM((CORES, hh, 128), f32),
            pltpu.VMEM((hh, CORES * sub), f32),
            pltpu.VMEM((hh, CORES * sub), f32),
            pltpu.VMEM((hh, CORES * sub), bf16),
            pltpu.VMEM((ii, sub), f32),
            pltpu.VMEM((ii, sub), f32),
            pltpu.VMEM((ii, sub), f32),
            pltpu.VMEM((ii, CORES * sub), bf16),
            pltpu.VMEM((ii, CORES * sub), bf16),
            pltpu.VMEM((hh, CORES * sub), bf16),
            pltpu.VMEM((2, 8, ii), f32),
            pltpu.VMEM((2, 8, ii), f32),
            pltpu.VMEM((hh, 128), f32),
            pltpu.VMEM((2, hh, ii), bf16),
            pltpu.VMEM((2, rows, hp, ip), bf16),
            pltpu.VMEM((2, rows, hp, ip), bf16),
            pltpu.VMEM((2, rows, hp, ip), bf16),
            pltpu.VMEM((2, rows, hp, ip), bf16),
            pltpu.VMEM((2, rows, hp, ip), bf16),
            pltpu.VMEM((2, rows, hp, ip), bf16),
            pltpu.SemaphoreType.DMA((80, rows)),
            pltpu.SemaphoreType.DMA((4,)),
        ],
        compiler_params=pltpu.CompilerParams(
            collective_id=0, has_side_effects=True, vmem_limit_bytes=60 * 1024 * 1024
        ),
    )(bucket, clean, noise, mod_table[0], w_first[0].T, w_second[0])
    return (out1.T[None], out2[None])


def solution(mesh):
    placed = (
        P("row", "col"),
        P("row", "col"),
        P(),
        P(),
        P(None, "row", "col"),
        P(None, "col", "row"),
    )
    return jax.shard_map(
        local_step if mesh.shape["col"] == CORES * SIDE * SIDE else local,
        mesh=mesh,
        in_specs=placed,
        out_specs=(P(None, "row", "col"), P(None, "col", "row")),
        check_vma=False,
    )
```

```python
import math

import jax
import jax.numpy as jnp
from jax import lax
from jax.experimental import pallas as pl
from jax.experimental.pallas import tpu as pltpu
from jax.sharding import PartitionSpec as P

PIX = 256
BUCKETS = 32


MIX_WEIGHT = 0.3
KEEP_COEF = (1.0 - MIX_WEIGHT) / math.sqrt((1.0 - MIX_WEIGHT) ** 2 + MIX_WEIGHT**2)
ADD_COEF = MIX_WEIGHT / math.sqrt((1.0 - MIX_WEIGHT) ** 2 + MIX_WEIGHT**2)
SILU_GAIN = 1.0 / 0.596
CONTRACT_LEAD = (((0,), (0,)), ((), ()))
CONTRACT_TAIL = (((1,), (1,)), ((), ()))


def noise_levels(bucket):
    return jnp.exp(-3.0 + 5.0 * (bucket.astype(jnp.float32) + 0.5) / BUCKETS)


def silu_slope(values):
    sig = jax.nn.sigmoid(values)
    return sig * (1.0 + values * (1.0 - sig))


def bucket_gains(table, picked):
    onehot = (picked[:, None] == jnp.arange(table.shape[0], dtype=jnp.int32)[None, :]).astype(
        jnp.float32
    )
    return jnp.dot(
        onehot, table, precision=lax.Precision.HIGHEST, preferred_element_type=jnp.float32
    )


def local(clean, noise, bucket, mod_table, w_first, w_second):
    rows_size = lax.axis_size("row")
    row_at = lax.axis_index("row")
    col_at = lax.axis_index("col")
    samples = bucket.shape[0]
    own_rows = clean.shape[1]
    weight_first = w_first[0]
    weight_second = w_second[0]
    table = 1.0 + mod_table[0]
    col_first = jnp.sqrt(lax.psum(jnp.sum(weight_first * weight_first, axis=0), "row") + 1.0)
    col_second = jnp.sqrt(lax.psum(jnp.sum(weight_second * weight_second, axis=0), "col") + 1.0)
    normed_first = (weight_first / col_first[None, :]).astype(jnp.bfloat16)
    normed_second = (weight_second / col_second[None, :]).astype(jnp.bfloat16)
    chan_clean, chan_noise = (
        lax.all_to_all(
            clean.astype(jnp.bfloat16), "row", split_axis=1, concat_axis=0, tiled=True
        ).astype(clean.dtype),
        lax.all_to_all(
            noise.astype(jnp.bfloat16), "row", split_axis=1, concat_axis=0, tiled=True
        ).astype(noise.dtype),
    )
    local_clean = chan_clean.T
    local_noise = chan_noise.T
    sub_rows = own_rows // rows_size
    first_row = col_at * own_rows + row_at * sub_rows
    row_sample = (first_row + jnp.arange(sub_rows, dtype=jnp.int32)) // PIX
    row_bucket = jnp.take(bucket, row_sample)
    levels = noise_levels(row_bucket)[:, None]
    spread_root = jnp.sqrt(levels * levels + 0.25)
    state_own = ((local_clean + levels * local_noise) / spread_root).astype(jnp.bfloat16)
    target = local_clean * (2.0 * levels / spread_root) - local_noise * (0.5 / spread_root)
    gains = bucket_gains(table, row_bucket)
    part_first, part_second = (
        lax.all_gather(normed_first, "col", axis=1, tiled=True),
        lax.all_gather(normed_second, "col", axis=0, tiled=True),
    )
    full_first, full_second = (
        lax.all_gather(part_first, "row", axis=0, tiled=True),
        lax.all_gather(part_second, "row", axis=1, tiled=True),
    )
    pre_act = jnp.dot(state_own, full_first, preferred_element_type=jnp.float32)
    hidden = (jax.nn.silu(pre_act) * SILU_GAIN * gains).astype(jnp.bfloat16)
    branch = jnp.dot(hidden, full_second, preferred_element_type=jnp.float32)
    state_new = (KEEP_COEF * state_own.astype(jnp.float32) + ADD_COEF * branch).astype(jnp.bfloat16)
    grad_own = (state_new.astype(jnp.float32) - target) / samples
    dbranch = (ADD_COEF * grad_own).astype(jnp.bfloat16)
    gsecond_full = lax.dot_general(
        hidden, dbranch, CONTRACT_LEAD, preferred_element_type=jnp.float32
    )
    dhidden = lax.dot_general(
        dbranch, full_second, CONTRACT_TAIL, preferred_element_type=jnp.float32
    )
    dpre = (dhidden * gains * silu_slope(pre_act) * SILU_GAIN).astype(jnp.bfloat16)
    gfirst_full = lax.dot_general(
        state_own, dpre, CONTRACT_LEAD, preferred_element_type=jnp.float32
    )
    part_gfirst, part_gsecond = (
        lax.psum_scatter(
            gfirst_full.astype(jnp.bfloat16), "col", scatter_dimension=1, tiled=True
        ).astype(jnp.float32),
        lax.psum_scatter(
            gsecond_full.astype(jnp.bfloat16), "col", scatter_dimension=0, tiled=True
        ).astype(jnp.float32),
    )
    gfirst, gsecond = (
        lax.psum_scatter(
            part_gfirst.astype(jnp.bfloat16), "row", scatter_dimension=0, tiled=True
        ).astype(jnp.float32),
        lax.psum_scatter(
            part_gsecond.astype(jnp.bfloat16), "row", scatter_dimension=1, tiled=True
        ).astype(jnp.float32),
    )
    dot_first = lax.psum(jnp.sum(weight_first * gfirst, axis=0), "row")
    dot_second = lax.psum(jnp.sum(weight_second * gsecond, axis=0), "col")
    grad_first = gfirst / col_first[None, :] - weight_first * (dot_first / col_first**3)[None, :]
    grad_second = (
        gsecond / col_second[None, :] - weight_second * (dot_second / col_second**3)[None, :]
    )
    return (grad_first[None], grad_second[None])


CORES = 2
SIDE = 2
MESH = pl.DeviceIdType.MESH


def round_up(size, unit):
    return -(-size // unit) * unit


def twice(value):
    return jnp.concatenate([value, value], axis=1)


def packing(hb, ib):
    full = ib // 128 * 128
    carried = round_up(ib + 1, 128) - ib
    left = ib - full - carried
    group = round_up(-(-round_up(hb + 2, 16) * max(left, 1) // 128), 16)
    return full, carried, left, group


SINGLE = set(
    [f"s{kind}{m}" for kind in "abABCDEFPxy" for m in range(2)]
    + ["s" + kind for kind in "ftgpqnd"] + ["ra0", "rb0", "rP0", "rP1"]
    + ["sz_z00", "sz_z01", "sz_z1"]
)


def split_sum(total):
    high = total.astype(jnp.bfloat16)
    low = (total - high.astype(jnp.float32)).astype(jnp.bfloat16)
    return high, low


def step_kernel(
    hb, ib, samples, names, bucket, clean, noise, table, w1h, w2h, out1h, out2h,
    cl, no, w1f, w2f, sto, w, wt, st, tg, nrm, gain, pre, slp, hid, brk, brp, brr, dbr, db2, dpre,
    s2, d2, dot1, g, gt, ra0, ra1, sa0, sa1, rb0, rb1, rc0, rc1, pz0, pz1, rz0, rz1, out1, out2,
    sems, local_sems,
):
    ra, sa, rb, rc, pz, rz = (ra0, ra1), (sa0, sa1), (rb0, rb1), (rc0, rc1), (pz0, pz1), (rz0, rz1)
    rows = st.shape[0] // round_up(ib + 1, 128)
    hp, ip = round_up(hb + 2, 16), round_up(ib + 1, 128)
    chips = w.shape[1] // hp
    sub = tg.shape[1]
    hh, ii = chips * hp, rows * ip
    own_rows = cl.shape[1]
    full, carried, left, group = packing(hb, ib)
    tp = wt.shape[2]
    bf16, f32 = jnp.bfloat16, jnp.float32
    z = lax.axis_index("row")
    col = lax.axis_index("col")
    core = lax.rem(col, CORES)
    xy = col // CORES
    x, y = lax.rem(xy, SIDE), xy // SIDE
    xn = y * SIDE + (1 - x)
    yn = (1 - y) * SIDE + x
    dn = (1 - y) * SIDE + (1 - x)
    dev_x = (z, xn * CORES + core)
    dev_y = (z, yn * CORES + core)
    dev_p = (z, xy * CORES + 1 - core)
    up, down = (z + 1, col), (z - 1, col)
    ring = [lax.rem(z + k, rows) for k in range(rows)]
    side = 1 - 2 * (z // (rows // 2))
    steps = [lax.rem(z + side * k + rows, rows) for k in range(1, rows)]
    outer = z // (rows - 1) + (rows - 1 - z) // (rows - 1)
    near = [z, steps[0], outer * steps[1] + (1 - outer) * steps[2], outer * steps[2] + (1 - outer) * steps[1]]

    loads = []
    for k, (src, dst) in enumerate([(w1h, w1f), (w2h, w2f), (clean, cl), (noise, no)]):
        loads.append(pltpu.make_async_copy(src, dst, local_sems.at[k]))
        loads[-1].start()
    barrier = pltpu.get_barrier_semaphore()
    peers = [dev_x, dev_y, dev_p] + [(ring[k], col) for k in range(1, rows)]
    for peer in peers:
        pl.semaphore_signal(barrier, inc=1, device_id=peer, device_id_type=MESH)

    pending = []

    def sem(kind, at):
        count = 1 if kind in SINGLE else rows
        if kind not in names:
            names[kind] = sum(size for _, size in names.values()), count
        return sems.at[names[kind][0] + (0 if count == 1 else at)]

    def remote(src, dst, kind, at_send, at_recv, dev):
        return pltpu.make_async_remote_copy(
            src_ref=src, dst_ref=dst, send_sem=sem("s" + kind, at_send),
            recv_sem=sem("r" + kind.split("_")[-1], at_recv), device_id=dev, device_id_type=MESH,
        )

    def when(cond, fn):
        if cond is None:
            fn()
        else:
            pl.when(cond)(fn)

    def send(cond, *spec):
        when(cond, lambda: remote(*spec).start())
        if spec[2].startswith("z_") or "s" + spec[2] not in SINGLE:
            pending.append((cond, spec))

    def arrive(cond, dst, kind, at):
        flag = sem("r" + kind, at)
        when(cond, lambda: pltpu.make_async_remote_copy(
            src_ref=dst, dst_ref=dst, send_sem=flag, recv_sem=flag, device_id=dev_p, device_id_type=MESH,
        ).wait_recv())

    def span(start, size, unit):
        return pl.ds(pl.multiple_of(start, unit), size)

    def part_rows(m, p):
        size = hp if m == 0 else tp
        cut = round_up(size // 2, 16) if m == 0 else size // 2 // 16 * 16
        return (0, cut) if p == 0 else (cut, size - cut)

    def wblk(m, xyb, zb, p=None):
        lo, size = (0, hp if m == 0 else tp) if p is None else part_rows(m, p)
        if m == 1:
            return wt.at[xyb, zb, slice(lo, lo + size), :]
        return w.at[0, span(xyb * hp + lo, size, 16), span(zb * ip, ip, 128)]

    tile_lane = lax.broadcasted_iota(jnp.int32, (hp, 128), 1)

    def fold(tail):
        turned = pltpu.roll(tail, 128 - carried, 1)
        folded = jnp.zeros((group, 128), f32)
        for q in range(128 // left):
            piece = turned[q * group : min((q + 1) * group, hp), :]
            piece = jnp.pad(piece, ((0, group - piece.shape[0]), (0, 0)))
            piece = piece if q == 0 else pltpu.roll(piece, left * q, 1)
            folded = jnp.where(tile_lane[:group] // left == q, piece, folded)
        return turned, folded

    def unfold(top, folded):
        pieces = []
        for q in range(128 // left):
            piece = folded if q == 0 else pltpu.roll(folded, 128 - left * q, 1)
            pieces.append(piece[: min(group, hp - q * group), :])
        turned = jnp.where(tile_lane < left, jnp.concatenate(pieces, axis=0), top)
        tail = pltpu.roll(turned, carried, 1)
        return jnp.where(tile_lane < carried + left, tail, 0.0)

    def chan(zb, size=ib):
        return span(zb * ip, size, 16)

    def pix(zb):
        return span(zb * sub, sub, 128)

    mine, other = slice(0, sub), slice(sub, 2 * sub)

    for zb in range(rows):
        pad = slice(zb * ip + ib, (zb + 1) * ip)
        st[pad, :] = jnp.zeros((ip - ib, 2 * sub), bf16)
        tg[pad, :] = jnp.zeros((ip - ib, sub), bf16)

    line = lax.broadcasted_iota(jnp.int32, (hp, ip), 0)
    blocks = []
    for m, whole in enumerate((w1f, w2f)):
        loads[m].wait()
        block = jnp.pad(whole[...], ((0, hp - hb), (0, ip - ib)))
        if m == 0:
            total = jnp.sum(block * block, axis=1, keepdims=True)
            total = jnp.pad(jnp.broadcast_to(total, (hp, 128)), ((0, 256 - hp), (0, 0)))
            total = jnp.pad(total.T[:1, :], ((0, 0), (0, ip - 256)))
        else:
            total = jnp.sum(block * block, axis=0, keepdims=True)
        high, low = split_sum(total)
        block = jnp.where(line == hb, high.astype(f32), block)
        block = jnp.where(line == hb + 1, low.astype(f32), block)
        blocks.append(block)
    turned, folded = fold(blocks[1][:, full:])
    first_tail = jnp.where(tile_lane < ib - full, blocks[0][:, full:], turned)
    w[0, span(xy * hp, hp, 16), span(z * ip, full, 128)] = blocks[0][:, :full].astype(bf16)
    w[0, span(xy * hp, hp, 16), span(z * ip + full, 128, 128)] = first_tail.astype(bf16)
    for k in range(full // 128):
        wt[xy, z, k * hp : (k + 1) * hp, :] = blocks[1][:, k * 128 : (k + 1) * 128].astype(bf16)
    wt[xy, z, full // 128 * hp :, :] = folded.astype(bf16)
    pl.semaphore_wait(barrier, len(peers))

    def along_z(cond, m, zb, go_up, go_down, p=None):
        kind = f"z{m}{'' if p is None else p}"
        block = wblk(m, xy, zb, p)
        if go_up:
            send(both(cond, z + 1 < rows), block, block, kind, z, zb, up)
        if go_down:
            send(both(cond, z > 0), block, block, "z_" + kind, 0, zb, down)

    def gather_wait(kind, region):
        flag = sem(kind, 0)
        copies = pltpu.make_async_remote_copy(
            src_ref=region, dst_ref=region, send_sem=flag, recv_sem=flag, device_id=dev_p, device_id_type=MESH,
        )
        if kind[0] == "s":
            copies.wait_send()
        else:
            copies.wait_recv()

    def both(a, b):
        return b if a is None else jnp.logical_and(a, b)

    def across(cond, m, zb):
        send(cond, wblk(m, xy, zb), wblk(m, xy, zb), f"x{m}", zb, zb, dev_x)
        send(cond, wblk(m, xy, zb), wblk(m, xy, zb), f"y{m}", zb, zb, dev_y)

    def diagonal(cond, m, zb):
        arrive(cond, wblk(m, xn, zb), f"x{m}", zb)
        send(cond, wblk(m, xn, zb, 0), wblk(m, xn, zb, 0), f"a{m}", zb, zb, dev_y)
        arrive(cond, wblk(m, yn, zb), f"y{m}", zb)
        send(cond, wblk(m, yn, zb, 1), wblk(m, yn, zb, 1), f"b{m}", zb, zb, dev_x)

    def sides(d):
        return ((z - d >= 0, z - d, True, False), (z + d < rows, z + d, False, True))

    def hop(m, d, p=None, signs=(-1, 1)):
        kind = f"z{m}{'' if p is None else p}"
        for sign in signs:
            zb, zt = z + sign * side * d, z - sign * side
            inside = jnp.logical_and(zb >= 0, zb < rows)
            block = wblk(m, xy, zb, p)
            arrive(inside, block, kind, zb)
            if d < rows - 1:
                onward = jnp.logical_and(inside, jnp.logical_and(zt >= 0, zt < rows))
                send(onward, block, block, kind, zb, zb, (zt, col))

    def each_side(fn, m, d):
        if d == 0:
            fn(None, m, z)
        else:
            for cond, zb, _, _ in sides(d):
                fn(cond, m, zb)

    end = jnp.logical_or(z == 0, z == rows - 1)
    middle = jnp.logical_not(end)
    for p in range(2):
        along_z(None, 0, z, True, True, p)
    along_z(end, 1, z, True, True)
    for m in range(2):
        across(None, m, z)

    loads[2].wait()
    loads[3].wait()
    for k in range(rows):
        lanes = slice(k * sub, (k + 1) * sub)
        picked = jnp.full((1, sub), bucket[col * rows + k], jnp.int32)
        level = noise_levels(picked)
        root = jnp.sqrt(level * level + 0.25)
        c, n = cl[:, lanes], no[:, lanes]
        sto[0, :, lanes] = ((c + level * n) / root).astype(bf16)
        sto[1, :, lanes] = (c * (2.0 * level / root) - n * (0.5 / root)).astype(bf16)
    st[chan(z), mine] = sto[0, :, pix(z)]
    tg[chan(z), :] = sto[1, :, pix(z)]

    def state_to_partner(zb):
        send(None, st.at[chan(zb), mine], st.at[chan(zb), other], "f", zb, zb, dev_p)

    def toward(kind, first, d):
        plane, target = (0, st.at[chan(z), mine]) if kind == "t" else (1, tg.at[chan(z), :])
        for direction, steps in ((1, z), (-1, rows - 1 - z)):
            zt = z + direction * d
            send(steps == first, sto.at[plane, :, pix(zt)], target,
                 kind, 0, z, (zt, col))

    def some(fn, wanted, m, d):
        for cond, zb, _, _ in sides(d):
            fn(jnp.logical_and(cond, wanted), m, zb)

    toward("t", 0, 1)
    state_to_partner(z)
    hop(0, 1, 0)
    hop(0, 1, 1)
    along_z(middle, 1, z, True, True)
    each_side(across, 0, 1)
    each_side(diagonal, 0, 0)
    hop(1, 1, None, (-1,))
    each_side(diagonal, 1, 0)
    hop(0, 2, 0)
    hop(0, 2, 1)
    each_side(across, 0, 2)
    hop(1, 1, None, (1,))
    toward("t", 1, 1)
    toward("t", 2, 1)
    each_side(diagonal, 0, 1)
    hop(0, 3, 0)
    hop(0, 3, 1)
    each_side(across, 0, 3)
    hop(1, 2)
    toward("t", 0, 2)
    toward("t", 1, 2)
    each_side(diagonal, 0, 2)
    each_side(across, 1, 1)
    each_side(across, 1, 2)
    toward("t", 0, 3)
    each_side(diagonal, 0, 3)
    hop(1, 3)
    each_side(across, 1, 3)
    toward("g", 1, 1)
    toward("g", 0, 1)
    stack = []
    for j in range(CORES):
        whose = core if j == 0 else 1 - core
        picked = bucket[(xy * CORES + whose) * rows + z]
        row = 1.0 + table[pl.ds(picked, 1), :]
        for b in range(chips):
            pieces = [row[:, (b * CORES + c) * hb : (b * CORES + c + 1) * hb] for c in range(CORES)]
            piece = jnp.where(core == 0, pieces[0], pieces[1])
            stack.append(jnp.pad(piece, ((0, 0), (0, 256 - hb))))
    def take_state(k):
        zb = near[k]
        arrive(None, st.at[chan(zb), mine], "t", zb)
        state_to_partner(zb)

    take_state(1)
    for p in range(2):
        lo, size = part_rows(0, p)
        gather_wait(f"r{'ab'[p]}0", w.at[0, span(dn * hp + lo, size, 16), :])

    def sums_of(m, b, lanes):
        tail = w[m, (b + 1) * hp - 16 : (b + 1) * hp, lanes].astype(f32)
        at = hb - (hp - 16)
        return tail[at : at + 1, :] + tail[at + 1 : at + 2, :]

    for b in range(chips):
        stack.append(sum(sums_of(0, b, slice(zb * ip, zb * ip + 256)) for zb in range(rows)))
    filler = 128 - len(stack)
    columns = jnp.concatenate(stack + [jnp.zeros((filler, 256), f32)], axis=0).T
    for b in range(chips):
        at = slice(b * hp, (b + 1) * hp)
        for j in range(CORES):
            k = j * chips + b
            gain[j, at, :] = jnp.broadcast_to(columns[:hp, k : k + 1], (hp, 128))
        k = CORES * chips + b
        nrm[at, :] = jnp.broadcast_to(jnp.sqrt(1.0 + columns[:hp, k : k + 1]), (hp, 128))
    half_rows = hh // 2

    def forward(k):
        zb = near[k]
        arrive(None, st.at[chan(zb), other], "f", zb)
        at_in = span(zb * ip, ip, 128)
        for part in range(2):
            at = slice(part * half_rows, (part + 1) * half_rows)
            value = jnp.dot(w[0, at, at_in], st[at_in, :], preferred_element_type=f32)
            if k > 0:
                value = value + pre[at, :]
            if k < rows - 1:
                pre[at, :] = value
                continue
            inverse = twice(1.0 / nrm[at, :])
            for j in range(CORES):
                lanes = slice(j * sub, (j + 1) * sub)
                v = value[:, lanes] * inverse
                sig = jax.nn.sigmoid(v)
                scale = twice(gain[j, at, :]) * SILU_GAIN
                pre[at, lanes] = v
                hid[at, lanes] = (v * sig * scale).astype(bf16)
                slp[at, lanes] = sig * (1.0 + v * (1.0 - sig)) * scale

    def zlanes(zb):
        return span(zb * ip, ip, 128)

    def branch_part(i):
        zb = near[i]
        at = zlanes(zb)
        arrive(None, wblk(1, dn, zb, 0), "a1", zb)
        arrive(None, wblk(1, dn, zb, 1), "b1", zb)
        for b in range(chips):
            rows_at = slice(b * hp, (b + 1) * hp)
            for k in range(full // 128):
                w[1, rows_at, span(zb * ip + k * 128, 128, 128)] = wt[b, zb, k * hp : (k + 1) * hp, :]
            tail_at = span(zb * ip + full, 128, 128)
            tail = unfold(w[0, rows_at, tail_at].astype(f32), wt[b, zb, full // 128 * hp :, :].astype(f32))
            w[1, rows_at, tail_at] = tail.astype(bf16)
        total = sum(sums_of(1, b, at) for b in range(chips))
        s2[0, :, at] = jnp.broadcast_to(total, (s2.shape[1], ip))
        send(None, s2.at[0, :, at], s2.at[1, :, at], "n", i, zb, dev_p)
        partial = lax.dot_general(w[1, :, at], hid[...], CONTRACT_LEAD, preferred_element_type=f32)
        brp[at, :] = partial[:, other]
        send(None, brp.at[at, :], brr.at[at, :], "p", i, zb, dev_p)
        brk[at, :] = partial[:, mine]

    def slope_part(i):
        zb = near[i]
        at = zlanes(zb)
        if i > 0:
            arrive(None, tg.at[chan(zb), :], "g", zb)
        arrive(None, s2.at[1, :, at], "n", zb)
        total = 1.0 + s2[0, :1, at] + s2[1, :1, at]
        norm = jnp.sqrt(jnp.broadcast_to(total, (128, ip)).T)
        inverse = 1.0 / norm
        arrive(None, brr.at[at, :], "p", zb)
        branch = (brk[at, :] + brr[at, :]) * twice(inverse)
        fresh = (KEEP_COEF * st[at, mine].astype(f32) + ADD_COEF * branch).astype(bf16)
        slope = (fresh.astype(f32) - tg[at, :].astype(f32)) / samples
        rounded = (ADD_COEF * slope).astype(bf16)
        dbr[at, mine] = rounded
        send(None, dbr.at[at, mine], dbr.at[at, other], "q", i, zb, dev_p)
        wide_rounded = rounded.astype(f32)
        db2[at, mine] = (wide_rounded * twice(inverse)).astype(bf16)
        product = jnp.sum(branch * wide_rounded, axis=1, keepdims=True) * norm
        d2[0, :, at] = product.T[: d2.shape[1], :]
        send(None, d2.at[0, :, at], d2.at[1, :, at], "d", i, zb, dev_p)

    hidden_line = lax.broadcasted_iota(jnp.int32, (hp, 1), 0)

    def second_part(i):
        zb = near[i]
        at = zlanes(zb)
        arrive(None, dbr.at[at, other], "q", zb)
        arrive(None, d2.at[1, :, at], "d", zb)
        second = lax.dot_general(hid[...], dbr[at, :], CONTRACT_TAIL, preferred_element_type=f32)
        dot2 = d2[0, :1, at] + d2[1, :1, at]
        for b in range(chips):
            rows_at = slice(b * hp, (b + 1) * hp)
            part = jnp.where(hidden_line >= hb, dot2, second[rows_at, :])
            for k in range(full // 128):
                gt[b, i, k * hp : (k + 1) * hp, :] = part[:, k * 128 : (k + 1) * 128].astype(bf16)
            turned, folded = fold(part[:, full:])
            gt[b, i, full // 128 * hp :, :] = folded.astype(bf16)
            g[rows_at, span(zb * ip + full, 128, 128)] = turned.astype(bf16)
        total = jnp.broadcast_to(1.0 + s2[0, :1, at] + s2[1, :1, at], (128, ip))
        inverse = 1.0 / jnp.sqrt(total.T)
        db2[at, other] = (dbr[at, other].astype(f32) * twice(inverse)).astype(bf16)

    dot_rows = []

    def backward():
        for part in range(2):
            at = slice(part * half_rows, (part + 1) * half_rows)
            grad = jnp.dot(w[1, at, :], db2[...], preferred_element_type=f32)
            rounded = (grad * slp[at, :]).astype(bf16)
            dpre[at, :] = rounded
            total = jnp.sum(rounded.astype(f32) * pre[at, :], axis=1, keepdims=True)
            dot1[at, :] = total * nrm[at, :]
        for b in range(chips):
            column = jnp.pad(dot1[b * hp : (b + 1) * hp, :], ((0, 256 - hp), (0, 0)))
            dot_rows.append(jnp.pad(column.T[:1, :], ((0, 0), (0, ip - 256))))

    lane = lax.broadcasted_iota(jnp.int32, (1, ip), 1)
    last = near[:0:-1] + [z]
    orders = (last, near)

    def first_part(i):
        zb = last[i]
        at = zlanes(zb)
        first = lax.dot_general(dpre[...], st[at, :], CONTRACT_TAIL, preferred_element_type=f32)
        tail_at = span(zb * ip + full, 128, 128)
        for b in range(chips):
            rows_at = slice(b * hp, (b + 1) * hp)
            part = jnp.where(hidden_line >= hb, dot_rows[b], first[rows_at, :])
            g[rows_at, span(zb * ip, full, 128)] = part[:, :full].astype(bf16)
            turned = g[rows_at, tail_at].astype(f32)
            g[rows_at, tail_at] = jnp.where(tile_lane < ib - full, part[:, full:], turned).astype(bf16)

    def gblk(m, xyb, i, p):
        lo, size = part_rows(m, p)
        if m == 1:
            return gt, (xyb, i, slice(lo, lo + size), slice(None))
        return g, (span(xyb * hp + lo, size, 16), span(last[i] * ip, ip, 128))

    def gref(m, xyb, i, p):
        ref, at = gblk(m, xyb, i, p)
        return ref.at[at]

    def gval(m, xyb, i, p):
        ref, at = gblk(m, xyb, i, p)
        return ref[at].astype(f32)

    def rblk_all(refs, m, lo, size):
        return refs[m].at[:, slice(lo, lo + size), :]

    def rblk(refs, m, i, p):
        lo, size = part_rows(m, p)
        return refs[m].at[i, slice(lo, lo + size), :]

    def legs(p):
        return (yn, dev_y, xn, dev_x) if p == 0 else (xn, dev_x, yn, dev_y)

    def stage_a(m, i):
        for p in range(2):
            nb1, dev1, nb2, dev2 = legs(p)
            send(None, gref(m, dn, i, p), rblk(ra, m, i, p), f"{'AB'[p]}{m}", i, i, dev1)
        for p in range(2):
            nb1, dev1, nb2, dev2 = legs(p)
            send(None, gref(m, nb1, i, p), rblk(rc, m, i, p), f"{'CD'[p]}{m}", i, i, dev1)

    def stage_b(m, i):
        for p in range(2):
            nb1, dev1, nb2, dev2 = legs(p)
            arrive(None, rblk(ra, m, i, p), f"{'AB'[p]}{m}", i)
            lo, size = part_rows(m, p)
            inside = (i, slice(lo, lo + size))
            sa[m][inside] = (gval(m, nb2, i, p) + ra[m][inside].astype(f32)).astype(bf16)
            send(None, rblk(sa, m, i, p), rblk(rb, m, i, p), f"{'EF'[p]}{m}", i, i, dev2)

    def stage_c(m, i):
        totals = []
        for p in range(2):
            arrive(None, rblk(rc, m, i, p), f"{'CD'[p]}{m}", i)
            arrive(None, rblk(rb, m, i, p), f"{'EF'[p]}{m}", i)
            lo, size = part_rows(m, p)
            inside = (i, slice(lo, lo + size))
            totals.append(gval(m, xy, i, p) + rb[m][inside].astype(f32) + rc[m][inside].astype(f32))
        own_at = rows - 1 if m == 0 else 0
        total = jnp.concatenate(totals, axis=0)
        if i == own_at:
            return total
        zb = orders[m][i]
        pz[m][i] = total.astype(bf16)
        send(None, pz[m].at[i], rz[m].at[z], f"P{m}", i, z, (zb, col))
        return None

    sums = [None, None]
    forward(0)
    forward(1)
    some(diagonal, end, 1, 1)
    take_state(2)
    take_state(3)
    toward("g", 2, 1)
    forward(2)
    forward(3)
    toward("g", 0, 2)
    toward("g", 1, 2)
    some(diagonal, middle, 1, 1)
    some(diagonal, end, 1, 2)
    branch_part(0)
    some(diagonal, middle, 1, 2)
    each_side(diagonal, 1, 3)
    slope_part(0)
    toward("g", 0, 3)
    second_part(0)
    stage_a(1, 0)
    branch_part(1)
    branch_part(2)
    slope_part(1)
    branch_part(3)
    second_part(1)
    stage_a(1, 1)
    slope_part(2)
    second_part(2)
    stage_a(1, 2)
    stage_b(1, 1)
    slope_part(3)
    second_part(3)
    stage_a(1, 3)
    backward()
    stage_b(1, 2)
    first_part(0)
    stage_a(0, 0)
    first_part(1)
    stage_b(1, 3)
    stage_a(0, 1)
    stage_c(1, 1)
    first_part(2)
    stage_b(0, 0)
    stage_a(0, 2)
    stage_c(1, 2)
    first_part(3)
    stage_b(0, 1)
    stage_c(1, 3)
    stage_c(0, 0)
    stage_b(0, 2)
    stage_a(0, 3)
    stage_b(1, 0)
    stage_c(0, 1)
    stage_c(0, 2)
    stage_b(0, 3)
    sums[1] = stage_c(1, 0)

    def collect(m, total):
        gather_wait(f"rP{m}", pz[m].at[0 : rows - 1])
        for k in range(1, rows):
            total = total + rz[m][ring[k]].astype(f32)
        return total

    second = collect(1, sums[1])
    norm2 = jnp.sqrt(1.0 + s2[0, :1, zlanes(z)] + s2[1, :1, zlanes(z)])[:, :ib]
    norm1 = nrm[span(xy * hp, hp, 16), :1][:hb]
    stores = [pltpu.make_async_copy(a, b, local_sems.at[4 + k])
              for k, (a, b) in enumerate(((out1, out1h), (out2, out2h)))]
    first = collect(0, stage_c(0, 3))

    def finish():
        row = jnp.broadcast_to(first[hb : hb + 1, :256], (128, 256))
        dot_first = row.T[:hb, :1]
        out1[...] = first[:hb, :ib] / norm1 - w1f[...] * (dot_first / (norm1 * norm1 * norm1))
        stores[0].start()
        tail = unfold(first[:, full:], second[full // 128 * hp :, :])
        both_tiles = [second[k * hp : (k + 1) * hp, :] for k in range(full // 128)]
        unpacked = jnp.concatenate(both_tiles + [tail], axis=1)
        dot_second = unpacked[hb : hb + 1, :ib]
        out2[...] = unpacked[:hb, :ib] / norm2 - w2f[...] * (dot_second / (norm2 * norm2 * norm2))
        stores[1].start()

    finish()
    for cond, spec in pending:
        when(cond, lambda spec=spec: remote(*spec).wait_send())
    for m in range(2):
        for p in range(2):
            lo, size = part_rows(m, p)
            region = rblk_all(rb, m, lo, size)
            for kind in ("ab"[p], "AB"[p], "CD"[p], "EF"[p]):
                gather_wait(f"s{kind}{m}", region)
        gather_wait(f"sP{m}", pz[m].at[0 : rows - 1])
    for kind in ("x", "y"):
        gather_wait(f"s{kind}0", w.at[0, :, 0:ip])
        gather_wait(f"s{kind}1", wt.at[0])
    gather_wait("sf", st.at[0 : rows * ib, mine])
    gather_wait("st", st.at[0 : (rows - 1) * ib, mine])
    gather_wait("sg", st.at[0 : (rows - 1) * ib, mine])
    gather_wait("sp", brp)
    gather_wait("sq", dbr.at[:, mine])
    gather_wait("sn", s2.at[0])
    gather_wait("sd", d2.at[0])
    stores[0].wait()
    stores[1].wait()
    used = sum(size for _, size in names.values())
    assert used == sems.shape[0], (used, sum(size == 1 for _, size in names.values()))


def local_step(clean, noise, bucket, mod_table, w_first, w_second):
    rows = lax.axis_size("row")
    cols = lax.axis_size("col")
    samples = bucket.shape[0]
    own_rows = clean.shape[1]
    ib, hb = clean.shape[0], w_first.shape[2]
    sub = own_rows // rows
    full, carried, left, group = packing(hb, ib)
    if sub != PIX or rows != 4 or left <= 0 or 128 % left != 0 or hb + 2 > 256:
        return local(clean, noise, bucket, mod_table, w_first, w_second)
    chips = cols // CORES
    hp, ip = round_up(hb + 2, 16), round_up(ib + 1, 128)
    bf16, f32 = jnp.bfloat16, jnp.float32
    hh, ii = chips * hp, rows * ip
    tp = full // 128 * hp + group
    vmem = pl.BlockSpec(memory_space=pltpu.VMEM)
    smem = pl.BlockSpec(memory_space=pltpu.SMEM)
    anywhere = pl.BlockSpec(memory_space=pl.ANY)
    out1, out2 = pl.pallas_call(
        lambda *refs: step_kernel(hb, ib, samples, {}, *refs),
        out_shape=(jax.ShapeDtypeStruct((hb, ib), f32), jax.ShapeDtypeStruct((hb, ib), f32)),
        in_specs=[smem, anywhere, anywhere, vmem, anywhere, anywhere],
        out_specs=(anywhere, anywhere),
        scratch_shapes=[
            pltpu.VMEM((ib, own_rows), f32),
            pltpu.VMEM((ib, own_rows), f32),
            pltpu.VMEM((hb, ib), f32),
            pltpu.VMEM((hb, ib), f32),
            pltpu.VMEM((2, ib, own_rows), bf16),
            pltpu.VMEM((2, hh, ii), bf16),
            pltpu.VMEM((chips, rows, tp, 128), bf16),
            pltpu.VMEM((ii, CORES * sub), bf16),
            pltpu.VMEM((ii, sub), bf16),
            pltpu.VMEM((hh, 128), f32),
            pltpu.VMEM((CORES, hh, 128), f32),
            pltpu.VMEM((hh, CORES * sub), f32),
            pltpu.VMEM((hh, CORES * sub), f32),
            pltpu.VMEM((hh, CORES * sub), bf16),
            pltpu.VMEM((ii, sub), f32),
            pltpu.VMEM((ii, sub), f32),
            pltpu.VMEM((ii, sub), f32),
            pltpu.VMEM((ii, CORES * sub), bf16),
            pltpu.VMEM((ii, CORES * sub), bf16),
            pltpu.VMEM((hh, CORES * sub), bf16),
            pltpu.VMEM((2, 8, ii), f32),
            pltpu.VMEM((2, 8, ii), f32),
            pltpu.VMEM((hh, 128), f32),
            pltpu.VMEM((hh, ii), bf16),
            pltpu.VMEM((chips, rows, tp, 128), bf16),
            pltpu.VMEM((rows, hp, ip), bf16),
            pltpu.VMEM((rows, tp, 128), bf16),
            pltpu.VMEM((rows, hp, ip), bf16),
            pltpu.VMEM((rows, tp, 128), bf16),
            pltpu.VMEM((rows, hp, ip), bf16),
            pltpu.VMEM((rows, tp, 128), bf16),
            pltpu.VMEM((rows, hp, ip), bf16),
            pltpu.VMEM((rows, tp, 128), bf16),
            pltpu.VMEM((rows, hp, ip), bf16),
            pltpu.VMEM((rows, tp, 128), bf16),
            pltpu.VMEM((rows, hp, ip), bf16),
            pltpu.VMEM((rows, tp, 128), bf16),
            pltpu.VMEM((hb, ib), f32),
            pltpu.VMEM((hb, ib), f32),
            pltpu.SemaphoreType.DMA((31 * rows + 36,)),
            pltpu.SemaphoreType.DMA((6,)),
        ],
        compiler_params=pltpu.CompilerParams(
            collective_id=0, has_side_effects=True, vmem_limit_bytes=60 * 1024 * 1024
        ),
    )(bucket, clean, noise, mod_table[0], w_first[0].T, w_second[0])
    return (out1.T[None], out2[None])


def solution(mesh):
    placed = (
        P("row", "col"),
        P("row", "col"),
        P(),
        P(),
        P(None, "row", "col"),
        P(None, "col", "row"),
    )
    return jax.shard_map(
        local_step if mesh.shape["col"] == CORES * SIDE * SIDE else local,
        mesh=mesh,
        in_specs=placed,
        out_specs=(P(None, "row", "col"), P(None, "col", "row")),
        check_vma=False,
    )
```

```python
import math

import jax
import jax.numpy as jnp
from jax import lax
from jax.experimental import pallas as pl
from jax.experimental.pallas import tpu as pltpu
from jax.sharding import PartitionSpec as P

PIX = 256
BUCKETS = 32


MIX_WEIGHT = 0.3
KEEP_COEF = (1.0 - MIX_WEIGHT) / math.sqrt((1.0 - MIX_WEIGHT) ** 2 + MIX_WEIGHT**2)
ADD_COEF = MIX_WEIGHT / math.sqrt((1.0 - MIX_WEIGHT) ** 2 + MIX_WEIGHT**2)
SILU_GAIN = 1.0 / 0.596
CONTRACT_LEAD = (((0,), (0,)), ((), ()))
CONTRACT_TAIL = (((1,), (1,)), ((), ()))


def noise_levels(bucket):
    return jnp.exp(-3.0 + 5.0 * (bucket.astype(jnp.float32) + 0.5) / BUCKETS)


def silu_slope(values):
    sig = jax.nn.sigmoid(values)
    return sig * (1.0 + values * (1.0 - sig))


def bucket_gains(table, picked):
    onehot = (picked[:, None] == jnp.arange(table.shape[0], dtype=jnp.int32)[None, :]).astype(
        jnp.float32
    )
    return jnp.dot(
        onehot, table, precision=lax.Precision.HIGHEST, preferred_element_type=jnp.float32
    )


def local(clean, noise, bucket, mod_table, w_first, w_second):
    rows_size = lax.axis_size("row")
    row_at = lax.axis_index("row")
    col_at = lax.axis_index("col")
    samples = bucket.shape[0]
    own_rows = clean.shape[1]
    weight_first = w_first[0]
    weight_second = w_second[0]
    table = 1.0 + mod_table[0]
    col_first = jnp.sqrt(lax.psum(jnp.sum(weight_first * weight_first, axis=0), "row") + 1.0)
    col_second = jnp.sqrt(lax.psum(jnp.sum(weight_second * weight_second, axis=0), "col") + 1.0)
    normed_first = (weight_first / col_first[None, :]).astype(jnp.bfloat16)
    normed_second = (weight_second / col_second[None, :]).astype(jnp.bfloat16)
    chan_clean, chan_noise = (
        lax.all_to_all(
            clean.astype(jnp.bfloat16), "row", split_axis=1, concat_axis=0, tiled=True
        ).astype(clean.dtype),
        lax.all_to_all(
            noise.astype(jnp.bfloat16), "row", split_axis=1, concat_axis=0, tiled=True
        ).astype(noise.dtype),
    )
    local_clean = chan_clean.T
    local_noise = chan_noise.T
    sub_rows = own_rows // rows_size
    first_row = col_at * own_rows + row_at * sub_rows
    row_sample = (first_row + jnp.arange(sub_rows, dtype=jnp.int32)) // PIX
    row_bucket = jnp.take(bucket, row_sample)
    levels = noise_levels(row_bucket)[:, None]
    spread_root = jnp.sqrt(levels * levels + 0.25)
    state_own = ((local_clean + levels * local_noise) / spread_root).astype(jnp.bfloat16)
    target = local_clean * (2.0 * levels / spread_root) - local_noise * (0.5 / spread_root)
    gains = bucket_gains(table, row_bucket)
    part_first, part_second = (
        lax.all_gather(normed_first, "col", axis=1, tiled=True),
        lax.all_gather(normed_second, "col", axis=0, tiled=True),
    )
    full_first, full_second = (
        lax.all_gather(part_first, "row", axis=0, tiled=True),
        lax.all_gather(part_second, "row", axis=1, tiled=True),
    )
    pre_act = jnp.dot(state_own, full_first, preferred_element_type=jnp.float32)
    hidden = (jax.nn.silu(pre_act) * SILU_GAIN * gains).astype(jnp.bfloat16)
    branch = jnp.dot(hidden, full_second, preferred_element_type=jnp.float32)
    state_new = (KEEP_COEF * state_own.astype(jnp.float32) + ADD_COEF * branch).astype(jnp.bfloat16)
    grad_own = (state_new.astype(jnp.float32) - target) / samples
    dbranch = (ADD_COEF * grad_own).astype(jnp.bfloat16)
    gsecond_full = lax.dot_general(
        hidden, dbranch, CONTRACT_LEAD, preferred_element_type=jnp.float32
    )
    dhidden = lax.dot_general(
        dbranch, full_second, CONTRACT_TAIL, preferred_element_type=jnp.float32
    )
    dpre = (dhidden * gains * silu_slope(pre_act) * SILU_GAIN).astype(jnp.bfloat16)
    gfirst_full = lax.dot_general(
        state_own, dpre, CONTRACT_LEAD, preferred_element_type=jnp.float32
    )
    part_gfirst, part_gsecond = (
        lax.psum_scatter(
            gfirst_full.astype(jnp.bfloat16), "col", scatter_dimension=1, tiled=True
        ).astype(jnp.float32),
        lax.psum_scatter(
            gsecond_full.astype(jnp.bfloat16), "col", scatter_dimension=0, tiled=True
        ).astype(jnp.float32),
    )
    gfirst, gsecond = (
        lax.psum_scatter(
            part_gfirst.astype(jnp.bfloat16), "row", scatter_dimension=0, tiled=True
        ).astype(jnp.float32),
        lax.psum_scatter(
            part_gsecond.astype(jnp.bfloat16), "row", scatter_dimension=1, tiled=True
        ).astype(jnp.float32),
    )
    dot_first = lax.psum(jnp.sum(weight_first * gfirst, axis=0), "row")
    dot_second = lax.psum(jnp.sum(weight_second * gsecond, axis=0), "col")
    grad_first = gfirst / col_first[None, :] - weight_first * (dot_first / col_first**3)[None, :]
    grad_second = (
        gsecond / col_second[None, :] - weight_second * (dot_second / col_second**3)[None, :]
    )
    return (grad_first[None], grad_second[None])


CORES = 2
SIDE = 2
MESH = pl.DeviceIdType.MESH


def round_up(size, unit):
    return -(-size // unit) * unit


def twice(value):
    return jnp.concatenate([value, value], axis=1)


def packing(hb, ib):
    full = ib // 128 * 128
    carried = round_up(ib + 1, 128) - ib
    left = ib - full - carried
    group = round_up(-(-round_up(hb + 2, 16) * max(left, 1) // 128), 16)
    return full, carried, left, group


SINGLE = set(
    [f"s{kind}{m}" for kind in "abABCDEFPxy" for m in range(2)]
    + ["s" + kind for kind in "ftgpqnd"] + ["ra0", "rb0", "rP0", "rP1"]
    + ["sz_z00", "sz_z01", "sz_z1"]
)


def split_sum(total):
    high = total.astype(jnp.bfloat16)
    low = (total - high.astype(jnp.float32)).astype(jnp.bfloat16)
    return high, low


def step_kernel(
    hb, ib, samples, names, bucket_h, clean, noise, table_h, w1h, w2h, out1h, out2h,
    cl, no, w1f, w2f, sto, w, wt, st, tg, nrm, gain, pre, slp, hid, brk, brp, brr, dbr, db2, dpre,
    s2, d2, dot1, g, gt, ra0, ra1, sa0, sa1, rb0, rb1, rc0, rc1, pz0, pz1, rz0, rz1, out1, out2,
    bucket, table, sems, local_sems,
):
    ra, sa, rb, rc, pz, rz = (ra0, ra1), (sa0, sa1), (rb0, rb1), (rc0, rc1), (pz0, pz1), (rz0, rz1)
    rows = st.shape[0] // round_up(ib + 1, 128)
    hp, ip = round_up(hb + 2, 16), round_up(ib + 1, 128)
    chips = w.shape[1] // hp
    sub = tg.shape[1]
    hh, ii = chips * hp, rows * ip
    own_rows = cl.shape[1]
    full, carried, left, group = packing(hb, ib)
    tp = wt.shape[2]
    bf16, f32 = jnp.bfloat16, jnp.float32
    z = lax.axis_index("row")
    col = lax.axis_index("col")
    core = lax.rem(col, CORES)
    xy = col // CORES
    x, y = lax.rem(xy, SIDE), xy // SIDE
    xn = y * SIDE + (1 - x)
    yn = (1 - y) * SIDE + x
    dn = (1 - y) * SIDE + (1 - x)
    dev_x = (z, xn * CORES + core)
    dev_y = (z, yn * CORES + core)
    dev_p = (z, xy * CORES + 1 - core)
    up, down = (z + 1, col), (z - 1, col)
    ring = [lax.rem(z + k, rows) for k in range(rows)]
    side = 1 - 2 * (z // (rows // 2))
    steps = [lax.rem(z + side * k + rows, rows) for k in range(1, rows)]
    outer = z // (rows - 1) + (rows - 1 - z) // (rows - 1)
    near = [z] + [outer * steps[k] + (1 - outer) * steps[(k + 2) % 3] for k in range(3)]

    loads = []
    for k, (src, dst) in enumerate([
        (w1h, w1f), (w2h, w2f), (clean, cl), (noise, no), (bucket_h, bucket), (table_h, table)
    ]):
        loads.append(pltpu.make_async_copy(src, dst, local_sems.at[k]))
        loads[-1].start()
    barrier = pltpu.get_barrier_semaphore()
    peers = [dev_x, dev_y, dev_p] + [(ring[k], col) for k in range(1, rows)]
    for peer in peers:
        pl.semaphore_signal(barrier, inc=1, device_id=peer, device_id_type=MESH)

    pending = []

    def sem(kind, at):
        count = 1 if kind in SINGLE else rows
        if kind not in names:
            names[kind] = sum(size for _, size in names.values()), count
        return sems.at[names[kind][0] + (0 if count == 1 else at)]

    def remote(src, dst, kind, at_send, at_recv, dev):
        return pltpu.make_async_remote_copy(
            src_ref=src, dst_ref=dst, send_sem=sem("s" + kind, at_send),
            recv_sem=sem("r" + kind.split("_")[-1], at_recv), device_id=dev, device_id_type=MESH,
        )

    def when(cond, fn):
        if cond is None:
            fn()
        else:
            pl.when(cond)(fn)

    def send(cond, *spec):
        when(cond, lambda: remote(*spec).start())
        if spec[2].startswith("z_") or "s" + spec[2] not in SINGLE:
            pending.append((cond, spec))

    def arrive(cond, dst, kind, at):
        flag = sem("r" + kind, at)
        when(cond, lambda: pltpu.make_async_remote_copy(
            src_ref=dst, dst_ref=dst, send_sem=flag, recv_sem=flag, device_id=dev_p, device_id_type=MESH,
        ).wait_recv())

    def span(start, size, unit):
        return pl.ds(pl.multiple_of(start, unit), size)

    def part_rows(m, p):
        size = hp if m == 0 else tp
        cut = round_up(size // 2, 16) if m == 0 else size // 2 // 16 * 16
        return (0, cut) if p == 0 else (cut, size - cut)

    def wblk(m, xyb, zb, p=None):
        lo, size = (0, hp if m == 0 else tp) if p is None else part_rows(m, p)
        if m == 1:
            return wt.at[xyb, zb, slice(lo, lo + size), :]
        return w.at[0, span(xyb * hp + lo, size, 16), span(zb * ip, ip, 128)]

    tile_lane = lax.broadcasted_iota(jnp.int32, (hp, 128), 1)

    def fold(tail):
        turned = pltpu.roll(tail, 128 - carried, 1)
        folded = jnp.zeros((group, 128), f32)
        for q in range(128 // left):
            piece = turned[q * group : min((q + 1) * group, hp), :]
            piece = jnp.pad(piece, ((0, group - piece.shape[0]), (0, 0)))
            piece = piece if q == 0 else pltpu.roll(piece, left * q, 1)
            folded = jnp.where(tile_lane[:group] // left == q, piece, folded)
        return turned, folded

    def unfold(top, folded):
        pieces = []
        for q in range(128 // left):
            piece = folded if q == 0 else pltpu.roll(folded, 128 - left * q, 1)
            pieces.append(piece[: min(group, hp - q * group), :])
        turned = jnp.where(tile_lane < left, jnp.concatenate(pieces, axis=0), top)
        tail = pltpu.roll(turned, carried, 1)
        return jnp.where(tile_lane < carried + left, tail, 0.0)

    def chan(zb, size=ib):
        return span(zb * ip, size, 16)

    def pix(zb):
        return span(zb * sub, sub, 128)

    mine, other = slice(0, sub), slice(sub, 2 * sub)

    for zb in range(rows):
        pad = slice(zb * ip + ib, (zb + 1) * ip)
        st[pad, :] = jnp.zeros((ip - ib, 2 * sub), bf16)
        tg[pad, :] = jnp.zeros((ip - ib, sub), bf16)

    line = lax.broadcasted_iota(jnp.int32, (hp, ip), 0)
    blocks = []
    for m, whole in enumerate((w1f, w2f)):
        loads[m].wait()
        block = jnp.pad(whole[...], ((0, hp - hb), (0, ip - ib)))
        if m == 0:
            total = jnp.sum(block * block, axis=1, keepdims=True)
            total = jnp.pad(jnp.broadcast_to(total, (hp, 128)), ((0, 256 - hp), (0, 0)))
            total = jnp.pad(total.T[:1, :], ((0, 0), (0, ip - 256)))
        else:
            total = jnp.sum(block * block, axis=0, keepdims=True)
        high, low = split_sum(total)
        block = jnp.where(line == hb, high.astype(f32), block)
        block = jnp.where(line == hb + 1, low.astype(f32), block)
        blocks.append(block)
    turned, folded = fold(blocks[1][:, full:])
    first_tail = jnp.where(tile_lane < ib - full, blocks[0][:, full:], turned)
    w[0, span(xy * hp, hp, 16), span(z * ip, full, 128)] = blocks[0][:, :full].astype(bf16)
    w[0, span(xy * hp, hp, 16), span(z * ip + full, 128, 128)] = first_tail.astype(bf16)
    for k in range(full // 128):
        wt[xy, z, k * hp : (k + 1) * hp, :] = blocks[1][:, k * 128 : (k + 1) * 128].astype(bf16)
    wt[xy, z, full // 128 * hp :, :] = folded.astype(bf16)
    pl.semaphore_wait(barrier, len(peers))

    def along_z(cond, m, zb, go_up, go_down, p=None):
        kind = f"z{m}{'' if p is None else p}"
        block = wblk(m, xy, zb, p)
        if go_up:
            send(both(cond, z + 1 < rows), block, block, kind, z, zb, up)
        if go_down:
            send(both(cond, z > 0), block, block, "z_" + kind, 0, zb, down)

    def gather_wait(kind, region):
        flag = sem(kind, 0)
        copies = pltpu.make_async_remote_copy(
            src_ref=region, dst_ref=region, send_sem=flag, recv_sem=flag, device_id=dev_p, device_id_type=MESH,
        )
        if kind[0] == "s":
            copies.wait_send()
        else:
            copies.wait_recv()

    def both(a, b):
        return b if a is None else jnp.logical_and(a, b)

    def across(cond, m, zb):
        send(cond, wblk(m, xy, zb), wblk(m, xy, zb), f"x{m}", zb, zb, dev_x)
        send(cond, wblk(m, xy, zb), wblk(m, xy, zb), f"y{m}", zb, zb, dev_y)

    def diagonal(cond, m, zb):
        arrive(cond, wblk(m, xn, zb), f"x{m}", zb)
        send(cond, wblk(m, xn, zb, 0), wblk(m, xn, zb, 0), f"a{m}", zb, zb, dev_y)
        arrive(cond, wblk(m, yn, zb), f"y{m}", zb)
        send(cond, wblk(m, yn, zb, 1), wblk(m, yn, zb, 1), f"b{m}", zb, zb, dev_x)

    def sides(d):
        found = []
        for sign in (-1, 1):
            zb = z + sign * side * d
            found.append((jnp.logical_and(zb >= 0, zb < rows), zb))
        return found

    def hop(m, d, p=None, signs=(-1, 1), who=None):
        kind = f"z{m}{'' if p is None else p}"
        for sign in signs:
            zb, zt = z + sign * side * d, z - sign * side
            inside = jnp.logical_and(zb >= 0, zb < rows)
            inside = inside if who is None else jnp.logical_and(inside, who)
            block = wblk(m, xy, zb, p)
            arrive(inside, block, kind, zb)
            if d < rows - 1:
                onward = jnp.logical_and(inside, jnp.logical_and(zt >= 0, zt < rows))
                send(onward, block, block, kind, zb, zb, (zt, col))

    def each_side(fn, m, d):
        if d == 0:
            fn(None, m, z)
        else:
            for cond, zb in sides(d):
                fn(cond, m, zb)

    end = jnp.logical_or(z == 0, z == rows - 1)
    middle = jnp.logical_not(end)
    for p in range(2):
        along_z(None, 0, z, True, True, p)
    along_z(end, 1, z, True, True)
    for m in range(2):
        across(None, m, z)

    loads[2].wait()
    loads[3].wait()
    loads[4].wait()
    loads[5].wait()
    for k in range(rows):
        lanes = slice(k * sub, (k + 1) * sub)
        picked = jnp.full((1, sub), bucket[col * rows + k], jnp.int32)
        level = noise_levels(picked)
        root = jnp.sqrt(level * level + 0.25)
        c, n = cl[:, lanes], no[:, lanes]
        sto[0, :, lanes] = ((c + level * n) / root).astype(bf16)
        sto[1, :, lanes] = (c * (2.0 * level / root) - n * (0.5 / root)).astype(bf16)
    st[chan(z), mine] = sto[0, :, pix(z)]
    tg[chan(z), :] = sto[1, :, pix(z)]

    def state_to_partner(zb):
        send(None, st.at[chan(zb), mine], st.at[chan(zb), other], "f", zb, zb, dev_p)

    def toward(kind, first, d):
        plane, target = (0, st.at[chan(z), mine]) if kind == "t" else (1, tg.at[chan(z), :])
        for direction, steps in ((1, z), (-1, rows - 1 - z)):
            zt = z + direction * d
            send(steps == first, sto.at[plane, :, pix(zt)], target,
                 kind, 0, z, (zt, col))

    def some(fn, wanted, m, d):
        for cond, zb in sides(d):
            fn(jnp.logical_and(cond, wanted), m, zb)

    toward("t", 0, 1)
    state_to_partner(z)
    hop(0, 1, 0)
    hop(0, 1, 1)
    along_z(middle, 1, z, True, True)
    each_side(across, 0, 1)
    each_side(diagonal, 0, 0)
    hop(1, 1, None, (-1,))
    hop(0, 2, 0)
    hop(0, 2, 1)
    each_side(across, 0, 2)
    hop(1, 1, None, (1,))
    toward("t", 1, 1)
    toward("t", 2, 1)
    each_side(diagonal, 0, 1)
    each_side(diagonal, 1, 0)
    hop(0, 3, 0)
    hop(0, 3, 1)
    each_side(across, 0, 3)
    toward("t", 0, 2)
    hop(1, 2, None, (-1, 1), middle)
    toward("t", 1, 2)
    each_side(diagonal, 0, 2)
    each_side(across, 1, 1)
    some(across, middle, 1, 2)
    each_side(diagonal, 0, 3)
    toward("t", 0, 3)
    hop(1, 2, None, (-1, 1), end)
    some(across, end, 1, 2)
    toward("g", 1, 1)
    toward("g", 0, 1)
    stack = []
    for j in range(CORES):
        whose = core if j == 0 else 1 - core
        picked = bucket[(xy * CORES + whose) * rows + z]
        row = 1.0 + table[pl.ds(picked, 1), :]
        for b in range(chips):
            pieces = [row[:, (b * CORES + c) * hb : (b * CORES + c + 1) * hb] for c in range(CORES)]
            piece = jnp.where(core == 0, pieces[0], pieces[1])
            stack.append(jnp.pad(piece, ((0, 0), (0, 256 - hb))))
    def take_state(k):
        zb = near[k]
        arrive(None, st.at[chan(zb), mine], "t", zb)
        state_to_partner(zb)

    take_state(1)
    for p in range(2):
        lo, size = part_rows(0, p)
        gather_wait(f"r{'ab'[p]}0", w.at[0, span(dn * hp + lo, size, 16), :])

    def sums_of(m, b, lanes):
        tail = w[m, (b + 1) * hp - 16 : (b + 1) * hp, lanes].astype(f32)
        at = hb - (hp - 16)
        return tail[at : at + 1, :] + tail[at + 1 : at + 2, :]

    for b in range(chips):
        stack.append(sum(sums_of(0, b, slice(zb * ip, zb * ip + 256)) for zb in range(rows)))
    filler = 128 - len(stack)
    columns = jnp.concatenate(stack + [jnp.zeros((filler, 256), f32)], axis=0).T
    for b in range(chips):
        at = slice(b * hp, (b + 1) * hp)
        for j in range(CORES):
            k = j * chips + b
            gain[j, at, :] = jnp.broadcast_to(columns[:hp, k : k + 1], (hp, 128))
        k = CORES * chips + b
        nrm[at, :] = jnp.broadcast_to(jnp.sqrt(1.0 + columns[:hp, k : k + 1]), (hp, 128))
    half_rows = hh // 2

    def forward(k):
        zb = near[k]
        arrive(None, st.at[chan(zb), other], "f", zb)
        at_in = span(zb * ip, ip, 128)
        for part in range(2):
            at = slice(part * half_rows, (part + 1) * half_rows)
            value = jnp.dot(w[0, at, at_in], st[at_in, :], preferred_element_type=f32)
            if k > 0:
                value = value + pre[at, :]
            if k < rows - 1:
                pre[at, :] = value
                continue
            inverse = twice(1.0 / nrm[at, :])
            for j in range(CORES):
                lanes = slice(j * sub, (j + 1) * sub)
                v = value[:, lanes] * inverse
                sig = jax.nn.sigmoid(v)
                scale = twice(gain[j, at, :]) * SILU_GAIN
                pre[at, lanes] = v
                hid[at, lanes] = (v * sig * scale).astype(bf16)
                slp[at, lanes] = sig * (1.0 + v * (1.0 - sig)) * scale

    def zlanes(zb):
        return span(zb * ip, ip, 128)

    def open_second(i):
        zb = near[i]
        at = zlanes(zb)
        arrive(None, wblk(1, dn, zb, 0), "a1", zb)
        arrive(None, wblk(1, dn, zb, 1), "b1", zb)
        for b in range(chips):
            rows_at = slice(b * hp, (b + 1) * hp)
            for k in range(full // 128):
                w[1, rows_at, span(zb * ip + k * 128, 128, 128)] = wt[b, zb, k * hp : (k + 1) * hp, :]
            tail_at = span(zb * ip + full, 128, 128)
            tail = unfold(w[0, rows_at, tail_at].astype(f32), wt[b, zb, full // 128 * hp :, :].astype(f32))
            w[1, rows_at, tail_at] = tail.astype(bf16)
        total = sum(sums_of(1, b, at) for b in range(chips))
        s2[0, :, at] = jnp.broadcast_to(total, (s2.shape[1], ip))
        send(None, s2.at[0, :, at], s2.at[1, :, at], "n", i, zb, dev_p)

    def branch_part(i):
        zb = near[i]
        at = zlanes(zb)
        partial = lax.dot_general(w[1, :, at], hid[...], CONTRACT_LEAD, preferred_element_type=f32)
        brp[at, :] = partial[:, other]
        send(None, brp.at[at, :], brr.at[at, :], "p", i, zb, dev_p)
        brk[at, :] = partial[:, mine]

    def slope_part(i):
        zb = near[i]
        at = zlanes(zb)
        if i > 0:
            arrive(None, tg.at[chan(zb), :], "g", zb)
        arrive(None, s2.at[1, :, at], "n", zb)
        total = 1.0 + s2[0, :1, at] + s2[1, :1, at]
        norm = jnp.sqrt(jnp.broadcast_to(total, (128, ip)).T)
        inverse = 1.0 / norm
        arrive(None, brr.at[at, :], "p", zb)
        branch = (brk[at, :] + brr[at, :]) * twice(inverse)
        fresh = (KEEP_COEF * st[at, mine].astype(f32) + ADD_COEF * branch).astype(bf16)
        slope = (fresh.astype(f32) - tg[at, :].astype(f32)) / samples
        rounded = (ADD_COEF * slope).astype(bf16)
        dbr[at, mine] = rounded
        send(None, dbr.at[at, mine], dbr.at[at, other], "q", i, zb, dev_p)
        wide_rounded = rounded.astype(f32)
        db2[at, mine] = (wide_rounded * twice(inverse)).astype(bf16)
        product = jnp.sum(branch * wide_rounded, axis=1, keepdims=True) * norm
        d2[0, :, at] = product.T[: d2.shape[1], :]
        send(None, d2.at[0, :, at], d2.at[1, :, at], "d", i, zb, dev_p)

    hidden_line = lax.broadcasted_iota(jnp.int32, (hp, 1), 0)

    def second_part(i):
        zb = near[i]
        at = zlanes(zb)
        if i == 0:
            second = lax.dot_general(hid[:, mine], dbr[at, mine], CONTRACT_TAIL, preferred_element_type=f32)
        arrive(None, dbr.at[at, other], "q", zb)
        arrive(None, d2.at[1, :, at], "d", zb)
        if i == 0:
            second = second + lax.dot_general(
                hid[:, other], dbr[at, other], CONTRACT_TAIL, preferred_element_type=f32
            )
        else:
            second = lax.dot_general(hid[...], dbr[at, :], CONTRACT_TAIL, preferred_element_type=f32)
        dot2 = d2[0, :1, at] + d2[1, :1, at]
        for b in range(chips):
            rows_at = slice(b * hp, (b + 1) * hp)
            part = jnp.where(hidden_line >= hb, dot2, second[rows_at, :])
            for k in range(full // 128):
                gt[b, i, k * hp : (k + 1) * hp, :] = part[:, k * 128 : (k + 1) * 128].astype(bf16)
            turned, folded = fold(part[:, full:])
            gt[b, i, full // 128 * hp :, :] = folded.astype(bf16)
            g[rows_at, span(zb * ip + full, 128, 128)] = turned.astype(bf16)
        total = jnp.broadcast_to(1.0 + s2[0, :1, at] + s2[1, :1, at], (128, ip))
        inverse = 1.0 / jnp.sqrt(total.T)
        db2[at, other] = (dbr[at, other].astype(f32) * twice(inverse)).astype(bf16)

    dot_rows = []

    def backward():
        for part in range(2):
            at = slice(part * half_rows, (part + 1) * half_rows)
            grad = jnp.dot(w[1, at, :], db2[...], preferred_element_type=f32)
            rounded = (grad * slp[at, :]).astype(bf16)
            dpre[at, :] = rounded
            total = jnp.sum(rounded.astype(f32) * pre[at, :], axis=1, keepdims=True)
            dot1[at, :] = total * nrm[at, :]
        for b in range(chips):
            column = jnp.pad(dot1[b * hp : (b + 1) * hp, :], ((0, 256 - hp), (0, 0)))
            dot_rows.append(jnp.pad(column.T[:1, :], ((0, 0), (0, ip - 256))))

    lane = lax.broadcasted_iota(jnp.int32, (1, ip), 1)
    last = near[:0:-1] + [z]
    orders = (last, near)

    def first_part(i):
        zb = last[i]
        at = zlanes(zb)
        first = lax.dot_general(dpre[...], st[at, :], CONTRACT_TAIL, preferred_element_type=f32)
        tail_at = span(zb * ip + full, 128, 128)
        for b in range(chips):
            rows_at = slice(b * hp, (b + 1) * hp)
            part = jnp.where(hidden_line >= hb, dot_rows[b], first[rows_at, :])
            g[rows_at, span(zb * ip, full, 128)] = part[:, :full].astype(bf16)
            turned = g[rows_at, tail_at].astype(f32)
            g[rows_at, tail_at] = jnp.where(tile_lane < ib - full, part[:, full:], turned).astype(bf16)

    def gblk(m, xyb, i, p):
        lo, size = part_rows(m, p)
        if m == 1:
            return gt, (xyb, i, slice(lo, lo + size), slice(None))
        return g, (span(xyb * hp + lo, size, 16), span(last[i] * ip, ip, 128))

    def gref(m, xyb, i, p):
        ref, at = gblk(m, xyb, i, p)
        return ref.at[at]

    def gval(m, xyb, i, p):
        ref, at = gblk(m, xyb, i, p)
        return ref[at].astype(f32)

    def rblk_all(refs, m, lo, size):
        return refs[m].at[:, slice(lo, lo + size), :]

    def rblk(refs, m, i, p):
        lo, size = part_rows(m, p)
        return refs[m].at[i, slice(lo, lo + size), :]

    def legs(p):
        return (yn, dev_y, xn, dev_x) if p == 0 else (xn, dev_x, yn, dev_y)

    def stage_a(m, i):
        for p in range(2):
            nb1, dev1, nb2, dev2 = legs(p)
            send(None, gref(m, dn, i, p), rblk(ra, m, i, p), f"{'AB'[p]}{m}", i, i, dev1)
        for p in range(2):
            nb1, dev1, nb2, dev2 = legs(p)
            send(None, gref(m, nb1, i, p), rblk(rc, m, i, p), f"{'CD'[p]}{m}", i, i, dev1)

    def stage_b(m, i):
        for p in range(2):
            nb1, dev1, nb2, dev2 = legs(p)
            arrive(None, rblk(ra, m, i, p), f"{'AB'[p]}{m}", i)
            lo, size = part_rows(m, p)
            inside = (i, slice(lo, lo + size))
            sa[m][inside] = (gval(m, nb2, i, p) + ra[m][inside].astype(f32)).astype(bf16)
            send(None, rblk(sa, m, i, p), rblk(rb, m, i, p), f"{'EF'[p]}{m}", i, i, dev2)

    def stage_c(m, i):
        totals = []
        for p in range(2):
            arrive(None, rblk(rc, m, i, p), f"{'CD'[p]}{m}", i)
            arrive(None, rblk(rb, m, i, p), f"{'EF'[p]}{m}", i)
            lo, size = part_rows(m, p)
            inside = (i, slice(lo, lo + size))
            totals.append(gval(m, xy, i, p) + rb[m][inside].astype(f32) + rc[m][inside].astype(f32))
        own_at = rows - 1 if m == 0 else 0
        total = jnp.concatenate(totals, axis=0)
        if i == own_at:
            return total
        zb = orders[m][i]
        pz[m][i] = total.astype(bf16)
        send(None, pz[m].at[i], rz[m].at[z], f"P{m}", i, z, (zb, col))
        return None

    sums = [None, None]
    forward(0)
    forward(1)
    hop(1, 3)
    each_side(across, 1, 3)
    some(diagonal, end, 1, 1)
    take_state(2)
    take_state(3)
    toward("g", 2, 1)
    open_second(0)
    forward(2)
    forward(3)
    toward("g", 0, 2)
    toward("g", 1, 2)
    some(diagonal, middle, 1, 1)
    some(diagonal, end, 1, 2)
    branch_part(0)
    some(diagonal, middle, 1, 2)
    each_side(diagonal, 1, 3)
    open_second(1)
    branch_part(1)
    slope_part(0)
    toward("g", 0, 3)
    slope_part(1)
    second_part(0)
    stage_a(1, 0)
    open_second(2)
    branch_part(2)
    second_part(1)
    stage_a(1, 1)
    open_second(3)
    branch_part(3)
    stage_b(1, 0)
    slope_part(2)
    second_part(2)
    stage_a(1, 2)
    stage_b(1, 1)
    slope_part(3)
    second_part(3)
    stage_a(1, 3)
    backward()
    stage_b(1, 2)
    first_part(0)
    stage_a(0, 0)
    first_part(1)
    stage_b(1, 3)
    stage_a(0, 1)
    stage_c(1, 1)
    first_part(2)
    stage_b(0, 0)
    stage_a(0, 2)
    stage_c(1, 2)
    first_part(3)
    stage_b(0, 1)
    stage_c(1, 3)
    stage_c(0, 0)
    stage_b(0, 2)
    stage_a(0, 3)
    stage_c(0, 1)
    stage_c(0, 2)
    stage_b(0, 3)
    sums[1] = stage_c(1, 0)

    def collect(m, total):
        gather_wait(f"rP{m}", pz[m].at[0 : rows - 1])
        for k in range(1, rows):
            total = total + rz[m][ring[k]].astype(f32)
        return total

    second = collect(1, sums[1])
    norm2 = jnp.sqrt(1.0 + s2[0, :1, zlanes(z)] + s2[1, :1, zlanes(z)])[:, :ib]
    norm1 = nrm[span(xy * hp, hp, 16), :1][:hb]
    stores = [pltpu.make_async_copy(a, b, local_sems.at[6 + k])
              for k, (a, b) in enumerate(((out1, out1h), (out2, out2h)))]
    first = collect(0, stage_c(0, 3))

    def finish():
        row = jnp.broadcast_to(first[hb : hb + 1, :256], (128, 256))
        dot_first = row.T[:hb, :1]
        out1[...] = first[:hb, :ib] / norm1 - w1f[...] * (dot_first / (norm1 * norm1 * norm1))
        stores[0].start()
        tail = unfold(first[:, full:], second[full // 128 * hp :, :])
        both_tiles = [second[k * hp : (k + 1) * hp, :] for k in range(full // 128)]
        unpacked = jnp.concatenate(both_tiles + [tail], axis=1)
        dot_second = unpacked[hb : hb + 1, :ib]
        out2[...] = unpacked[:hb, :ib] / norm2 - w2f[...] * (dot_second / (norm2 * norm2 * norm2))
        stores[1].start()

    finish()
    for cond, spec in pending:
        when(cond, lambda spec=spec: remote(*spec).wait_send())
    for m in range(2):
        for p in range(2):
            lo, size = part_rows(m, p)
            region = rblk_all(rb, m, lo, size)
            for kind in ("ab"[p], "AB"[p], "CD"[p], "EF"[p]):
                gather_wait(f"s{kind}{m}", region)
        gather_wait(f"sP{m}", pz[m].at[0 : rows - 1])
    for kind in ("x", "y"):
        gather_wait(f"s{kind}0", w.at[0, :, 0:ip])
        gather_wait(f"s{kind}1", wt.at[0])
    gather_wait("sf", st.at[0 : rows * ib, mine])
    gather_wait("st", st.at[0 : (rows - 1) * ib, mine])
    gather_wait("sg", st.at[0 : (rows - 1) * ib, mine])
    gather_wait("sp", brp)
    gather_wait("sq", dbr.at[:, mine])
    gather_wait("sn", s2.at[0])
    gather_wait("sd", d2.at[0])
    stores[0].wait()
    stores[1].wait()
    used = sum(size for _, size in names.values())
    assert used == sems.shape[0], (used, sum(size == 1 for _, size in names.values()))


def hand_over(in1, in2, out1, out2):
    out1[...] = in1[...]
    out2[...] = in2[...]


def local_step(clean, noise, bucket, mod_table, w_first, w_second):
    rows = lax.axis_size("row")
    cols = lax.axis_size("col")
    samples = bucket.shape[0]
    own_rows = clean.shape[1]
    ib, hb = clean.shape[0], w_first.shape[2]
    sub = own_rows // rows
    full, carried, left, group = packing(hb, ib)
    if sub != PIX or rows != 4 or left <= 0 or 128 % left != 0 or hb + 2 > 256:
        return local(clean, noise, bucket, mod_table, w_first, w_second)
    chips = cols // CORES
    hp, ip = round_up(hb + 2, 16), round_up(ib + 1, 128)
    bf16, f32 = jnp.bfloat16, jnp.float32
    hh, ii = chips * hp, rows * ip
    tp = full // 128 * hp + group
    vmem = pl.BlockSpec(memory_space=pltpu.VMEM)
    anywhere = pl.BlockSpec(memory_space=pl.ANY)
    out1, out2 = pl.pallas_call(
        lambda *refs: step_kernel(hb, ib, samples, {}, *refs),
        out_shape=(jax.ShapeDtypeStruct((hb, ib), f32), jax.ShapeDtypeStruct((hb, ib), f32)),
        in_specs=[anywhere] * 6,
        out_specs=(anywhere, anywhere),
        scratch_shapes=[
            pltpu.VMEM((ib, own_rows), f32),
            pltpu.VMEM((ib, own_rows), f32),
            pltpu.VMEM((hb, ib), f32),
            pltpu.VMEM((hb, ib), f32),
            pltpu.VMEM((2, ib, own_rows), bf16),
            pltpu.VMEM((2, hh, ii), bf16),
            pltpu.VMEM((chips, rows, tp, 128), bf16),
            pltpu.VMEM((ii, CORES * sub), bf16),
            pltpu.VMEM((ii, sub), bf16),
            pltpu.VMEM((hh, 128), f32),
            pltpu.VMEM((CORES, hh, 128), f32),
            pltpu.VMEM((hh, CORES * sub), f32),
            pltpu.VMEM((hh, CORES * sub), f32),
            pltpu.VMEM((hh, CORES * sub), bf16),
            pltpu.VMEM((ii, sub), f32),
            pltpu.VMEM((ii, sub), f32),
            pltpu.VMEM((ii, sub), f32),
            pltpu.VMEM((ii, CORES * sub), bf16),
            pltpu.VMEM((ii, CORES * sub), bf16),
            pltpu.VMEM((hh, CORES * sub), bf16),
            pltpu.VMEM((2, 8, ii), f32),
            pltpu.VMEM((2, 8, ii), f32),
            pltpu.VMEM((hh, 128), f32),
            pltpu.VMEM((hh, ii), bf16),
            pltpu.VMEM((chips, rows, tp, 128), bf16),
            pltpu.VMEM((rows, hp, ip), bf16),
            pltpu.VMEM((rows, tp, 128), bf16),
            pltpu.VMEM((rows, hp, ip), bf16),
            pltpu.VMEM((rows, tp, 128), bf16),
            pltpu.VMEM((rows, hp, ip), bf16),
            pltpu.VMEM((rows, tp, 128), bf16),
            pltpu.VMEM((rows, hp, ip), bf16),
            pltpu.VMEM((rows, tp, 128), bf16),
            pltpu.VMEM((rows, hp, ip), bf16),
            pltpu.VMEM((rows, tp, 128), bf16),
            pltpu.VMEM((rows, hp, ip), bf16),
            pltpu.VMEM((rows, tp, 128), bf16),
            pltpu.VMEM((hb, ib), f32),
            pltpu.VMEM((hb, ib), f32),
            pltpu.SMEM(bucket.shape, jnp.int32),
            pltpu.VMEM(mod_table.shape[1:], f32),
            pltpu.SemaphoreType.DMA((31 * rows + 36,)),
            pltpu.SemaphoreType.DMA((8,)),
        ],
        compiler_params=pltpu.CompilerParams(
            collective_id=0, has_side_effects=True, vmem_limit_bytes=60 * 1024 * 1024
        ),
    )(bucket, clean, noise, mod_table[0], w_first[0].T, w_second[0])
    out1, out2 = pl.pallas_call(
        hand_over,
        out_shape=(jax.ShapeDtypeStruct((hb, ib), f32), jax.ShapeDtypeStruct((hb, ib), f32)),
        in_specs=[vmem] * 2,
        out_specs=(vmem, vmem),
    )(out1, out2)
    return (out1.T[None], out2[None])


def solution(mesh):
    placed = (
        P("row", "col"),
        P("row", "col"),
        P(),
        P(),
        P(None, "row", "col"),
        P(None, "col", "row"),
    )
    return jax.shard_map(
        local_step if mesh.shape["col"] == CORES * SIDE * SIDE else local,
        mesh=mesh,
        in_specs=placed,
        out_specs=(P(None, "row", "col"), P(None, "col", "row")),
        check_vma=False,
    )
```

```python
import math

import jax
import jax.numpy as jnp
from jax import lax
from jax.experimental import pallas as pl
from jax.experimental.pallas import tpu as pltpu
from jax.sharding import PartitionSpec as P

PIX = 256
BUCKETS = 32


MIX_WEIGHT = 0.3
KEEP_COEF = (1.0 - MIX_WEIGHT) / math.sqrt((1.0 - MIX_WEIGHT) ** 2 + MIX_WEIGHT**2)
ADD_COEF = MIX_WEIGHT / math.sqrt((1.0 - MIX_WEIGHT) ** 2 + MIX_WEIGHT**2)
SILU_GAIN = 1.0 / 0.596
CONTRACT_LEAD = (((0,), (0,)), ((), ()))
CONTRACT_TAIL = (((1,), (1,)), ((), ()))


def noise_levels(bucket):
    return jnp.exp(-3.0 + 5.0 * (bucket.astype(jnp.float32) + 0.5) / BUCKETS)


def silu_slope(values):
    sig = jax.nn.sigmoid(values)
    return sig * (1.0 + values * (1.0 - sig))


def bucket_gains(table, picked):
    onehot = (picked[:, None] == jnp.arange(table.shape[0], dtype=jnp.int32)[None, :]).astype(
        jnp.float32
    )
    return jnp.dot(
        onehot, table, precision=lax.Precision.HIGHEST, preferred_element_type=jnp.float32
    )


def local(clean, noise, bucket, mod_table, w_first, w_second):
    rows_size = lax.axis_size("row")
    row_at = lax.axis_index("row")
    col_at = lax.axis_index("col")
    samples = bucket.shape[0]
    own_rows = clean.shape[1]
    weight_first = w_first[0]
    weight_second = w_second[0]
    table = 1.0 + mod_table[0]
    col_first = jnp.sqrt(lax.psum(jnp.sum(weight_first * weight_first, axis=0), "row") + 1.0)
    col_second = jnp.sqrt(lax.psum(jnp.sum(weight_second * weight_second, axis=0), "col") + 1.0)
    normed_first = (weight_first / col_first[None, :]).astype(jnp.bfloat16)
    normed_second = (weight_second / col_second[None, :]).astype(jnp.bfloat16)
    chan_clean, chan_noise = (
        lax.all_to_all(
            clean.astype(jnp.bfloat16), "row", split_axis=1, concat_axis=0, tiled=True
        ).astype(clean.dtype),
        lax.all_to_all(
            noise.astype(jnp.bfloat16), "row", split_axis=1, concat_axis=0, tiled=True
        ).astype(noise.dtype),
    )
    local_clean = chan_clean.T
    local_noise = chan_noise.T
    sub_rows = own_rows // rows_size
    first_row = col_at * own_rows + row_at * sub_rows
    row_sample = (first_row + jnp.arange(sub_rows, dtype=jnp.int32)) // PIX
    row_bucket = jnp.take(bucket, row_sample)
    levels = noise_levels(row_bucket)[:, None]
    spread_root = jnp.sqrt(levels * levels + 0.25)
    state_own = ((local_clean + levels * local_noise) / spread_root).astype(jnp.bfloat16)
    target = local_clean * (2.0 * levels / spread_root) - local_noise * (0.5 / spread_root)
    gains = bucket_gains(table, row_bucket)
    part_first, part_second = (
        lax.all_gather(normed_first, "col", axis=1, tiled=True),
        lax.all_gather(normed_second, "col", axis=0, tiled=True),
    )
    full_first, full_second = (
        lax.all_gather(part_first, "row", axis=0, tiled=True),
        lax.all_gather(part_second, "row", axis=1, tiled=True),
    )
    pre_act = jnp.dot(state_own, full_first, preferred_element_type=jnp.float32)
    hidden = (jax.nn.silu(pre_act) * SILU_GAIN * gains).astype(jnp.bfloat16)
    branch = jnp.dot(hidden, full_second, preferred_element_type=jnp.float32)
    state_new = (KEEP_COEF * state_own.astype(jnp.float32) + ADD_COEF * branch).astype(jnp.bfloat16)
    grad_own = (state_new.astype(jnp.float32) - target) / samples
    dbranch = (ADD_COEF * grad_own).astype(jnp.bfloat16)
    gsecond_full = lax.dot_general(
        hidden, dbranch, CONTRACT_LEAD, preferred_element_type=jnp.float32
    )
    dhidden = lax.dot_general(
        dbranch, full_second, CONTRACT_TAIL, preferred_element_type=jnp.float32
    )
    dpre = (dhidden * gains * silu_slope(pre_act) * SILU_GAIN).astype(jnp.bfloat16)
    gfirst_full = lax.dot_general(
        state_own, dpre, CONTRACT_LEAD, preferred_element_type=jnp.float32
    )
    part_gfirst, part_gsecond = (
        lax.psum_scatter(
            gfirst_full.astype(jnp.bfloat16), "col", scatter_dimension=1, tiled=True
        ).astype(jnp.float32),
        lax.psum_scatter(
            gsecond_full.astype(jnp.bfloat16), "col", scatter_dimension=0, tiled=True
        ).astype(jnp.float32),
    )
    gfirst, gsecond = (
        lax.psum_scatter(
            part_gfirst.astype(jnp.bfloat16), "row", scatter_dimension=0, tiled=True
        ).astype(jnp.float32),
        lax.psum_scatter(
            part_gsecond.astype(jnp.bfloat16), "row", scatter_dimension=1, tiled=True
        ).astype(jnp.float32),
    )
    dot_first = lax.psum(jnp.sum(weight_first * gfirst, axis=0), "row")
    dot_second = lax.psum(jnp.sum(weight_second * gsecond, axis=0), "col")
    grad_first = gfirst / col_first[None, :] - weight_first * (dot_first / col_first**3)[None, :]
    grad_second = (
        gsecond / col_second[None, :] - weight_second * (dot_second / col_second**3)[None, :]
    )
    return (grad_first[None], grad_second[None])


CORES = 2
SIDE = 2
MESH = pl.DeviceIdType.MESH


def round_up(size, unit):
    return -(-size // unit) * unit


def twice(value):
    return jnp.concatenate([value, value], axis=1)


def packing(hb, ib):
    full = ib // 128 * 128
    carried = round_up(ib + 1, 128) - ib
    left = ib - full - carried
    group = round_up(-(-round_up(hb + 2, 16) * max(left, 1) // 128), 16)
    return full, carried, left, group


SINGLE = set(
    [f"s{kind}{m}" for kind in "abABCDEFPxy" for m in range(2)]
    + ["s" + kind for kind in "ftgpqnd"] + ["ra0", "rb0", "rP0", "rP1"]
    + ["sz_z00", "sz_z01", "sz_z1"]
)


def split_sum(total):
    high = total.astype(jnp.bfloat16)
    low = (total - high.astype(jnp.float32)).astype(jnp.bfloat16)
    return high, low


def step_kernel(
    hb, ib, samples, names, bucket_h, clean, noise, table_h, w1h, w2h, out1h, out2h,
    cl, no, w1f, w2f, sto, w, wt, st, tg, nrm, gain, pre, slp, hid, brk, brp, brr, dbr, db2, dpre,
    s2, d2, dot1, g, gt, ra0, ra1, sa0, sa1, rb0, rb1, rc0, rc1, pz0, pz1, rz0, rz1, out1, out2,
    bucket, table, sems, local_sems,
):
    ra, sa, rb, rc, pz, rz = (ra0, ra1), (sa0, sa1), (rb0, rb1), (rc0, rc1), (pz0, pz1), (rz0, rz1)
    rows = st.shape[0] // round_up(ib + 1, 128)
    hp, ip = round_up(hb + 2, 16), round_up(ib + 1, 128)
    chips = w.shape[1] // hp
    sub = tg.shape[1]
    hh, ii = chips * hp, rows * ip
    own_rows = cl.shape[1]
    full, carried, left, group = packing(hb, ib)
    tp = wt.shape[2]
    bf16, f32 = jnp.bfloat16, jnp.float32
    z = lax.axis_index("row")
    col = lax.axis_index("col")
    core = lax.rem(col, CORES)
    xy = col // CORES
    x, y = lax.rem(xy, SIDE), xy // SIDE
    xn = y * SIDE + (1 - x)
    yn = (1 - y) * SIDE + x
    dn = (1 - y) * SIDE + (1 - x)
    dev_x = (z, xn * CORES + core)
    dev_y = (z, yn * CORES + core)
    dev_p = (z, xy * CORES + 1 - core)
    up, down = (z + 1, col), (z - 1, col)
    ring = [lax.rem(z + k, rows) for k in range(rows)]
    side = 1 - 2 * (z // (rows // 2))
    steps = [lax.rem(z + side * k + rows, rows) for k in range(1, rows)]
    outer = z // (rows - 1) + (rows - 1 - z) // (rows - 1)
    near = [z] + [outer * steps[k] + (1 - outer) * steps[(k + 2) % 3] for k in range(3)]

    loads = []
    for k, (src, dst) in enumerate([
        (w1h, w1f), (w2h, w2f), (clean, cl), (noise, no), (bucket_h, bucket), (table_h, table)
    ]):
        loads.append(pltpu.make_async_copy(src, dst, local_sems.at[k]))
        loads[-1].start()
    barrier = pltpu.get_barrier_semaphore()
    peers = [dev_x, dev_y, dev_p] + [(ring[k], col) for k in range(1, rows)]
    for peer in peers:
        pl.semaphore_signal(barrier, inc=1, device_id=peer, device_id_type=MESH)

    pending = []

    def sem(kind, at):
        count = 1 if kind in SINGLE else rows
        if kind not in names:
            names[kind] = sum(size for _, size in names.values()), count
        return sems.at[names[kind][0] + (0 if count == 1 else at)]

    def remote(src, dst, kind, at_send, at_recv, dev):
        return pltpu.make_async_remote_copy(
            src_ref=src, dst_ref=dst, send_sem=sem("s" + kind, at_send),
            recv_sem=sem("r" + kind.split("_")[-1], at_recv), device_id=dev, device_id_type=MESH,
        )

    def when(cond, fn):
        if cond is None:
            fn()
        else:
            pl.when(cond)(fn)

    def send(cond, *spec):
        when(cond, lambda: remote(*spec).start())
        if spec[2].startswith("z_") or "s" + spec[2] not in SINGLE:
            pending.append((cond, spec))

    def arrive(cond, dst, kind, at):
        flag = sem("r" + kind, at)
        when(cond, lambda: pltpu.make_async_remote_copy(
            src_ref=dst, dst_ref=dst, send_sem=flag, recv_sem=flag, device_id=dev_p, device_id_type=MESH,
        ).wait_recv())

    def span(start, size, unit):
        return pl.ds(pl.multiple_of(start, unit), size)

    def part_rows(m, p):
        size = hp if m == 0 else tp
        cut = round_up(size // 2, 16) if m == 0 else size // 2 // 16 * 16
        return (0, cut) if p == 0 else (cut, size - cut)

    def wblk(m, xyb, zb, p=None):
        lo, size = (0, hp if m == 0 else tp) if p is None else part_rows(m, p)
        if m == 1:
            return wt.at[xyb, zb, slice(lo, lo + size), :]
        return w.at[0, span(xyb * hp + lo, size, 16), span(zb * ip, ip, 128)]

    tile_lane = lax.broadcasted_iota(jnp.int32, (hp, 128), 1)

    def fold(tail):
        turned = pltpu.roll(tail, 128 - carried, 1)
        folded = jnp.zeros((group, 128), f32)
        for q in range(128 // left):
            piece = turned[q * group : min((q + 1) * group, hp), :]
            piece = jnp.pad(piece, ((0, group - piece.shape[0]), (0, 0)))
            piece = piece if q == 0 else pltpu.roll(piece, left * q, 1)
            folded = jnp.where(tile_lane[:group] // left == q, piece, folded)
        return turned, folded

    def unfold(top, folded):
        pieces = []
        for q in range(128 // left):
            piece = folded if q == 0 else pltpu.roll(folded, 128 - left * q, 1)
            pieces.append(piece[: min(group, hp - q * group), :])
        turned = jnp.where(tile_lane < left, jnp.concatenate(pieces, axis=0), top)
        tail = pltpu.roll(turned, carried, 1)
        return jnp.where(tile_lane < carried + left, tail, 0.0)

    def chan(zb, size=ib):
        return span(zb * ip, size, 16)

    def pix(zb):
        return span(zb * sub, sub, 128)

    mine, other = slice(0, sub), slice(sub, 2 * sub)

    for zb in range(rows):
        pad = slice(zb * ip + ib, (zb + 1) * ip)
        st[pad, :] = jnp.zeros((ip - ib, 2 * sub), bf16)
        tg[pad, :] = jnp.zeros((ip - ib, sub), bf16)

    line = lax.broadcasted_iota(jnp.int32, (hp, ip), 0)
    blocks = []
    for m, whole in enumerate((w1f, w2f)):
        loads[m].wait()
        block = jnp.pad(whole[...], ((0, hp - hb), (0, ip - ib)))
        if m == 0:
            total = jnp.sum(block * block, axis=1, keepdims=True)
            total = jnp.pad(jnp.broadcast_to(total, (hp, 128)), ((0, 256 - hp), (0, 0)))
            total = jnp.pad(total.T[:1, :], ((0, 0), (0, ip - 256)))
        else:
            total = jnp.sum(block * block, axis=0, keepdims=True)
        high, low = split_sum(total)
        block = jnp.where(line == hb, high.astype(f32), block)
        block = jnp.where(line == hb + 1, low.astype(f32), block)
        blocks.append(block)
    turned, folded = fold(blocks[1][:, full:])
    first_tail = jnp.where(tile_lane < ib - full, blocks[0][:, full:], turned)
    w[0, span(xy * hp, hp, 16), span(z * ip, full, 128)] = blocks[0][:, :full].astype(bf16)
    w[0, span(xy * hp, hp, 16), span(z * ip + full, 128, 128)] = first_tail.astype(bf16)
    for k in range(full // 128):
        wt[xy, z, k * hp : (k + 1) * hp, :] = blocks[1][:, k * 128 : (k + 1) * 128].astype(bf16)
    wt[xy, z, full // 128 * hp :, :] = folded.astype(bf16)
    pl.semaphore_wait(barrier, len(peers))

    def along_z(cond, m, zb, go_up, go_down, p=None):
        kind = f"z{m}{'' if p is None else p}"
        block = wblk(m, xy, zb, p)
        if go_up:
            send(both(cond, z + 1 < rows), block, block, kind, z, zb, up)
        if go_down:
            send(both(cond, z > 0), block, block, "z_" + kind, 0, zb, down)

    def gather_wait(kind, region):
        flag = sem(kind, 0)
        copies = pltpu.make_async_remote_copy(
            src_ref=region, dst_ref=region, send_sem=flag, recv_sem=flag, device_id=dev_p, device_id_type=MESH,
        )
        if kind[0] == "s":
            copies.wait_send()
        else:
            copies.wait_recv()

    def both(a, b):
        return b if a is None else jnp.logical_and(a, b)

    def across(cond, m, zb):
        send(cond, wblk(m, xy, zb), wblk(m, xy, zb), f"x{m}", zb, zb, dev_x)
        send(cond, wblk(m, xy, zb), wblk(m, xy, zb), f"y{m}", zb, zb, dev_y)

    def diagonal(cond, m, zb):
        arrive(cond, wblk(m, xn, zb), f"x{m}", zb)
        send(cond, wblk(m, xn, zb, 0), wblk(m, xn, zb, 0), f"a{m}", zb, zb, dev_y)
        arrive(cond, wblk(m, yn, zb), f"y{m}", zb)
        send(cond, wblk(m, yn, zb, 1), wblk(m, yn, zb, 1), f"b{m}", zb, zb, dev_x)

    def sides(d):
        found = []
        for sign in (-1, 1):
            zb = z + sign * side * d
            found.append((jnp.logical_and(zb >= 0, zb < rows), zb))
        return found

    def hop(m, d, p=None, signs=(-1, 1), who=None):
        kind = f"z{m}{'' if p is None else p}"
        for sign in signs:
            zb, zt = z + sign * side * d, z - sign * side
            inside = jnp.logical_and(zb >= 0, zb < rows)
            inside = inside if who is None else jnp.logical_and(inside, who)
            block = wblk(m, xy, zb, p)
            arrive(inside, block, kind, zb)
            if d < rows - 1:
                onward = jnp.logical_and(inside, jnp.logical_and(zt >= 0, zt < rows))
                send(onward, block, block, kind, zb, zb, (zt, col))

    def each_side(fn, m, d):
        if d == 0:
            fn(None, m, z)
        else:
            for cond, zb in sides(d):
                fn(cond, m, zb)

    end = jnp.logical_or(z == 0, z == rows - 1)
    middle = jnp.logical_not(end)
    for p in range(2):
        along_z(None, 0, z, True, True, p)
    along_z(end, 1, z, True, True)
    for m in range(2):
        across(None, m, z)

    loads[2].wait()
    loads[3].wait()
    loads[4].wait()
    loads[5].wait()
    for k in range(rows):
        lanes = slice(k * sub, (k + 1) * sub)
        picked = jnp.full((1, sub), bucket[col * rows + k], jnp.int32)
        level = noise_levels(picked)
        root = jnp.sqrt(level * level + 0.25)
        c, n = cl[:, lanes], no[:, lanes]
        sto[0, :, lanes] = ((c + level * n) / root).astype(bf16)
        sto[1, :, lanes] = (c * (2.0 * level / root) - n * (0.5 / root)).astype(bf16)
    st[chan(z), mine] = sto[0, :, pix(z)]
    tg[chan(z), :] = sto[1, :, pix(z)]

    def state_to_partner(zb):
        send(None, st.at[chan(zb), mine], st.at[chan(zb), other], "f", zb, zb, dev_p)

    def toward(kind, first, d):
        plane, target = (0, st.at[chan(z), mine]) if kind == "t" else (1, tg.at[chan(z), :])
        for direction, steps in ((1, z), (-1, rows - 1 - z)):
            zt = z + direction * d
            send(steps == first, sto.at[plane, :, pix(zt)], target,
                 kind, 0, z, (zt, col))

    def some(fn, wanted, m, d):
        for cond, zb in sides(d):
            fn(jnp.logical_and(cond, wanted), m, zb)

    toward("t", 0, 1)
    state_to_partner(z)
    hop(0, 1, 0)
    hop(0, 1, 1)
    along_z(middle, 1, z, True, True)
    each_side(across, 0, 1)
    each_side(diagonal, 0, 0)
    hop(1, 1, None, (-1,))
    hop(0, 2, 0)
    hop(0, 2, 1)
    each_side(across, 0, 2)
    hop(1, 1, None, (1,))
    toward("t", 1, 1)
    toward("t", 2, 1)
    each_side(diagonal, 0, 1)
    each_side(diagonal, 1, 0)
    hop(0, 3, 0)
    hop(0, 3, 1)
    each_side(across, 0, 3)
    toward("t", 0, 2)
    hop(1, 2, None, (-1, 1), middle)
    toward("t", 1, 2)
    each_side(diagonal, 0, 2)
    each_side(across, 1, 1)
    some(across, middle, 1, 2)
    each_side(diagonal, 0, 3)
    toward("t", 0, 3)
    hop(1, 2, None, (-1, 1), end)
    some(across, end, 1, 2)
    toward("g", 1, 1)
    toward("g", 0, 1)
    stack = []
    for j in range(CORES):
        whose = core if j == 0 else 1 - core
        picked = bucket[(xy * CORES + whose) * rows + z]
        row = 1.0 + table[pl.ds(picked, 1), :]
        for b in range(chips):
            pieces = [row[:, (b * CORES + c) * hb : (b * CORES + c + 1) * hb] for c in range(CORES)]
            piece = jnp.where(core == 0, pieces[0], pieces[1])
            stack.append(jnp.pad(piece, ((0, 0), (0, 256 - hb))))
    def take_state(k):
        zb = near[k]
        arrive(None, st.at[chan(zb), mine], "t", zb)
        state_to_partner(zb)

    take_state(1)
    for p in range(2):
        lo, size = part_rows(0, p)
        gather_wait(f"r{'ab'[p]}0", w.at[0, span(dn * hp + lo, size, 16), :])

    def sums_of(m, b, lanes):
        tail = w[m, (b + 1) * hp - 16 : (b + 1) * hp, lanes].astype(f32)
        at = hb - (hp - 16)
        return tail[at : at + 1, :] + tail[at + 1 : at + 2, :]

    for b in range(chips):
        stack.append(sum(sums_of(0, b, slice(zb * ip, zb * ip + 256)) for zb in range(rows)))
    filler = 128 - len(stack)
    columns = jnp.concatenate(stack + [jnp.zeros((filler, 256), f32)], axis=0).T
    for b in range(chips):
        at = slice(b * hp, (b + 1) * hp)
        for j in range(CORES):
            k = j * chips + b
            gain[j, at, :] = jnp.broadcast_to(columns[:hp, k : k + 1], (hp, 128))
        k = CORES * chips + b
        nrm[at, :] = jnp.broadcast_to(jnp.sqrt(1.0 + columns[:hp, k : k + 1]), (hp, 128))
    half_rows = hh // 2

    def forward(k):
        zb = near[k]
        arrive(None, st.at[chan(zb), other], "f", zb)
        at_in = span(zb * ip, ip, 128)
        for part in range(2):
            at = slice(part * half_rows, (part + 1) * half_rows)
            value = jnp.dot(w[0, at, at_in], st[at_in, :], preferred_element_type=f32)
            if k > 0:
                value = value + pre[at, :]
            if k < rows - 1:
                pre[at, :] = value
                continue
            inverse = twice(1.0 / nrm[at, :])
            for j in range(CORES):
                lanes = slice(j * sub, (j + 1) * sub)
                v = value[:, lanes] * inverse
                sig = jax.nn.sigmoid(v)
                scale = twice(gain[j, at, :]) * SILU_GAIN
                pre[at, lanes] = v
                hid[at, lanes] = (v * sig * scale).astype(bf16)
                slp[at, lanes] = sig * (1.0 + v * (1.0 - sig)) * scale

    def zlanes(zb):
        return span(zb * ip, ip, 128)

    def open_second(i):
        zb = near[i]
        at = zlanes(zb)
        arrive(None, wblk(1, dn, zb, 0), "a1", zb)
        arrive(None, wblk(1, dn, zb, 1), "b1", zb)
        for b in range(chips):
            rows_at = slice(b * hp, (b + 1) * hp)
            for k in range(full // 128):
                w[1, rows_at, span(zb * ip + k * 128, 128, 128)] = wt[b, zb, k * hp : (k + 1) * hp, :]
            tail_at = span(zb * ip + full, 128, 128)
            tail = unfold(w[0, rows_at, tail_at].astype(f32), wt[b, zb, full // 128 * hp :, :].astype(f32))
            w[1, rows_at, tail_at] = tail.astype(bf16)
        total = sum(sums_of(1, b, at) for b in range(chips))
        s2[0, :, at] = jnp.broadcast_to(total, (s2.shape[1], ip))
        send(None, s2.at[0, :, at], s2.at[1, :, at], "n", i, zb, dev_p)

    def branch_part(i):
        zb = near[i]
        at = zlanes(zb)
        partial = lax.dot_general(w[1, :, at], hid[...], CONTRACT_LEAD, preferred_element_type=f32)
        brp[at, :] = partial[:, other]
        send(None, brp.at[at, :], brr.at[at, :], "p", i, zb, dev_p)
        brk[at, :] = partial[:, mine]

    def slope_part(i):
        zb = near[i]
        at = zlanes(zb)
        if i > 0:
            arrive(None, tg.at[chan(zb), :], "g", zb)
        arrive(None, s2.at[1, :, at], "n", zb)
        total = 1.0 + s2[0, :1, at] + s2[1, :1, at]
        norm = jnp.sqrt(jnp.broadcast_to(total, (128, ip)).T)
        inverse = 1.0 / norm
        arrive(None, brr.at[at, :], "p", zb)
        branch = (brk[at, :] + brr[at, :]) * twice(inverse)
        fresh = (KEEP_COEF * st[at, mine].astype(f32) + ADD_COEF * branch).astype(bf16)
        slope = (fresh.astype(f32) - tg[at, :].astype(f32)) / samples
        rounded = (ADD_COEF * slope).astype(bf16)
        dbr[at, mine] = rounded
        send(None, dbr.at[at, mine], dbr.at[at, other], "q", i, zb, dev_p)
        wide_rounded = rounded.astype(f32)
        db2[at, mine] = (wide_rounded * twice(inverse)).astype(bf16)
        product = jnp.sum(branch * wide_rounded, axis=1, keepdims=True) * norm
        d2[0, :, at] = product.T[: d2.shape[1], :]
        send(None, d2.at[0, :, at], d2.at[1, :, at], "d", i, zb, dev_p)

    hidden_line = lax.broadcasted_iota(jnp.int32, (hp, 1), 0)

    def second_part(i):
        zb = near[i]
        at = zlanes(zb)
        if i == 0:
            second = lax.dot_general(hid[:, mine], dbr[at, mine], CONTRACT_TAIL, preferred_element_type=f32)
        arrive(None, dbr.at[at, other], "q", zb)
        arrive(None, d2.at[1, :, at], "d", zb)
        if i == 0:
            second = second + lax.dot_general(
                hid[:, other], dbr[at, other], CONTRACT_TAIL, preferred_element_type=f32
            )
        else:
            second = lax.dot_general(hid[...], dbr[at, :], CONTRACT_TAIL, preferred_element_type=f32)
        dot2 = d2[0, :1, at] + d2[1, :1, at]
        for b in range(chips):
            rows_at = slice(b * hp, (b + 1) * hp)
            part = jnp.where(hidden_line >= hb, dot2, second[rows_at, :])
            for k in range(full // 128):
                gt[b, i, k * hp : (k + 1) * hp, :] = part[:, k * 128 : (k + 1) * 128].astype(bf16)
            turned, folded = fold(part[:, full:])
            gt[b, i, full // 128 * hp :, :] = folded.astype(bf16)
            g[rows_at, span(zb * ip + full, 128, 128)] = turned.astype(bf16)
        total = jnp.broadcast_to(1.0 + s2[0, :1, at] + s2[1, :1, at], (128, ip))
        inverse = 1.0 / jnp.sqrt(total.T)
        db2[at, other] = (dbr[at, other].astype(f32) * twice(inverse)).astype(bf16)

    dot_rows = []

    def backward():
        for part in range(2):
            at = slice(part * half_rows, (part + 1) * half_rows)
            grad = jnp.dot(w[1, at, :], db2[...], preferred_element_type=f32)
            rounded = (grad * slp[at, :]).astype(bf16)
            dpre[at, :] = rounded
            total = jnp.sum(rounded.astype(f32) * pre[at, :], axis=1, keepdims=True)
            dot1[at, :] = total * nrm[at, :]
        for b in range(chips):
            column = jnp.pad(dot1[b * hp : (b + 1) * hp, :], ((0, 256 - hp), (0, 0)))
            dot_rows.append(jnp.pad(column.T[:1, :], ((0, 0), (0, ip - 256))))

    lane = lax.broadcasted_iota(jnp.int32, (1, ip), 1)
    last = near[:0:-1] + [z]
    orders = (last, near)

    def first_part(i):
        zb = last[i]
        at = zlanes(zb)
        first = lax.dot_general(dpre[...], st[at, :], CONTRACT_TAIL, preferred_element_type=f32)
        tail_at = span(zb * ip + full, 128, 128)
        for b in range(chips):
            rows_at = slice(b * hp, (b + 1) * hp)
            part = jnp.where(hidden_line >= hb, dot_rows[b], first[rows_at, :])
            g[rows_at, span(zb * ip, full, 128)] = part[:, :full].astype(bf16)
            turned = g[rows_at, tail_at].astype(f32)
            g[rows_at, tail_at] = jnp.where(tile_lane < ib - full, part[:, full:], turned).astype(bf16)

    def gblk(m, xyb, i, p):
        lo, size = part_rows(m, p)
        if m == 1:
            return gt, (xyb, i, slice(lo, lo + size), slice(None))
        return g, (span(xyb * hp + lo, size, 16), span(last[i] * ip, ip, 128))

    def gref(m, xyb, i, p):
        ref, at = gblk(m, xyb, i, p)
        return ref.at[at]

    def gval(m, xyb, i, p):
        ref, at = gblk(m, xyb, i, p)
        return ref[at].astype(f32)

    def rblk_all(refs, m, lo, size):
        return refs[m].at[:, slice(lo, lo + size), :]

    def rblk(refs, m, i, p):
        lo, size = part_rows(m, p)
        return refs[m].at[i, slice(lo, lo + size), :]

    def legs(p):
        return (yn, dev_y, xn, dev_x) if p == 0 else (xn, dev_x, yn, dev_y)

    def stage_a(m, i):
        for p in range(2):
            nb1, dev1, nb2, dev2 = legs(p)
            send(None, gref(m, dn, i, p), rblk(ra, m, i, p), f"{'AB'[p]}{m}", i, i, dev1)
        for p in range(2):
            nb1, dev1, nb2, dev2 = legs(p)
            send(None, gref(m, nb1, i, p), rblk(rc, m, i, p), f"{'CD'[p]}{m}", i, i, dev1)

    def stage_b(m, i):
        for p in range(2):
            nb1, dev1, nb2, dev2 = legs(p)
            arrive(None, rblk(ra, m, i, p), f"{'AB'[p]}{m}", i)
            lo, size = part_rows(m, p)
            inside = (i, slice(lo, lo + size))
            sa[m][inside] = (gval(m, nb2, i, p) + ra[m][inside].astype(f32)).astype(bf16)
            send(None, rblk(sa, m, i, p), rblk(rb, m, i, p), f"{'EF'[p]}{m}", i, i, dev2)

    def stage_c(m, i):
        zb = orders[m][i]
        own = i == (rows - 1 if m == 0 else 0)
        totals = []
        for p in range(2):
            arrive(None, rblk(rc, m, i, p), f"{'CD'[p]}{m}", i)
            arrive(None, rblk(rb, m, i, p), f"{'EF'[p]}{m}", i)
            lo, size = part_rows(m, p)
            inside = (i, slice(lo, lo + size))
            total = gval(m, xy, i, p) + rb[m][inside].astype(f32) + rc[m][inside].astype(f32)
            if own:
                totals.append(total)
            else:
                pz[m][inside] = total.astype(bf16)
                send(None, rblk(pz, m, i, p), rz[m].at[z, slice(lo, lo + size), :], f"P{m}", i, z, (zb, col))
        if own:
            return jnp.concatenate(totals, axis=0)
        return None

    sums = [None, None]
    forward(0)
    forward(1)
    hop(1, 3)
    each_side(across, 1, 3)
    some(diagonal, end, 1, 1)
    take_state(2)
    take_state(3)
    toward("g", 2, 1)
    open_second(0)
    forward(2)
    forward(3)
    toward("g", 1, 2)
    some(diagonal, middle, 1, 1)
    some(diagonal, end, 1, 2)
    branch_part(0)
    toward("g", 0, 2)
    some(diagonal, middle, 1, 2)
    each_side(diagonal, 1, 3)
    open_second(1)
    branch_part(1)
    slope_part(0)
    toward("g", 0, 3)
    slope_part(1)
    second_part(0)
    stage_a(1, 0)
    open_second(2)
    branch_part(2)
    second_part(1)
    stage_a(1, 1)
    open_second(3)
    branch_part(3)
    stage_b(1, 0)
    slope_part(2)
    second_part(2)
    stage_a(1, 2)
    stage_b(1, 1)
    slope_part(3)
    second_part(3)
    stage_a(1, 3)
    backward()
    stage_b(1, 2)
    first_part(0)
    stage_a(0, 0)
    first_part(1)
    stage_b(1, 3)
    stage_a(0, 1)
    stage_c(1, 1)
    first_part(2)
    stage_b(0, 0)
    stage_a(0, 2)
    stage_c(1, 2)
    first_part(3)
    stage_b(0, 1)
    stage_c(1, 3)
    stage_c(0, 0)
    stage_b(0, 2)
    stage_a(0, 3)
    stage_c(0, 1)
    stage_c(0, 2)
    stage_b(0, 3)
    sums[1] = stage_c(1, 0)

    def collect(m, total):
        gather_wait(f"rP{m}", pz[m].at[0 : rows - 1])
        for k in range(1, rows):
            total = total + rz[m][ring[k]].astype(f32)
        return total

    second = collect(1, sums[1])
    norm2 = jnp.sqrt(1.0 + s2[0, :1, zlanes(z)] + s2[1, :1, zlanes(z)])[:, :ib]
    norm1 = nrm[span(xy * hp, hp, 16), :1][:hb]
    first = collect(0, stage_c(0, 3))

    def finish():
        row = jnp.broadcast_to(first[hb : hb + 1, :256], (128, 256))
        dot_first = row.T[:hb, :1]
        out1h[...] = first[:hb, :ib] / norm1 - w1f[...] * (dot_first / (norm1 * norm1 * norm1))
        tail = unfold(first[:, full:], second[full // 128 * hp :, :])
        both_tiles = [second[k * hp : (k + 1) * hp, :] for k in range(full // 128)]
        unpacked = jnp.concatenate(both_tiles + [tail], axis=1)
        dot_second = unpacked[hb : hb + 1, :ib]
        out2h[...] = unpacked[:hb, :ib] / norm2 - w2f[...] * (dot_second / (norm2 * norm2 * norm2))

    finish()
    for cond, spec in pending:
        when(cond, lambda spec=spec: remote(*spec).wait_send())
    for m in range(2):
        for p in range(2):
            lo, size = part_rows(m, p)
            region = rblk_all(rb, m, lo, size)
            for kind in ("ab"[p], "AB"[p], "CD"[p], "EF"[p]):
                gather_wait(f"s{kind}{m}", region)
        gather_wait(f"sP{m}", pz[m].at[0 : rows - 1])
    for kind in ("x", "y"):
        gather_wait(f"s{kind}0", w.at[0, :, 0:ip])
        gather_wait(f"s{kind}1", wt.at[0])
    gather_wait("sf", st.at[0 : rows * ib, mine])
    gather_wait("st", st.at[0 : (rows - 1) * ib, mine])
    gather_wait("sg", st.at[0 : (rows - 1) * ib, mine])
    gather_wait("sp", brp)
    gather_wait("sq", dbr.at[:, mine])
    gather_wait("sn", s2.at[0])
    gather_wait("sd", d2.at[0])
    used = sum(size for _, size in names.values())
    assert used == sems.shape[0], (used, sum(size == 1 for _, size in names.values()))


def hand_over(in1, in2, out1, out2):
    out1[...] = in1[...]
    out2[...] = in2[...]


def local_step(clean, noise, bucket, mod_table, w_first, w_second):
    rows = lax.axis_size("row")
    cols = lax.axis_size("col")
    samples = bucket.shape[0]
    own_rows = clean.shape[1]
    ib, hb = clean.shape[0], w_first.shape[2]
    sub = own_rows // rows
    full, carried, left, group = packing(hb, ib)
    if sub != PIX or rows != 4 or left <= 0 or 128 % left != 0 or hb + 2 > 256:
        return local(clean, noise, bucket, mod_table, w_first, w_second)
    chips = cols // CORES
    hp, ip = round_up(hb + 2, 16), round_up(ib + 1, 128)
    bf16, f32 = jnp.bfloat16, jnp.float32
    hh, ii = chips * hp, rows * ip
    tp = full // 128 * hp + group
    vmem = pl.BlockSpec(memory_space=pltpu.VMEM)
    anywhere = pl.BlockSpec(memory_space=pl.ANY)
    out1, out2 = pl.pallas_call(
        lambda *refs: step_kernel(hb, ib, samples, {}, *refs),
        out_shape=(pltpu.VMEM((hb, ib), f32), pltpu.VMEM((hb, ib), f32)),
        in_specs=[anywhere] * 6,
        out_specs=(vmem, vmem),
        scratch_shapes=[
            pltpu.VMEM((ib, own_rows), f32),
            pltpu.VMEM((ib, own_rows), f32),
            pltpu.VMEM((hb, ib), f32),
            pltpu.VMEM((hb, ib), f32),
            pltpu.VMEM((2, ib, own_rows), bf16),
            pltpu.VMEM((2, hh, ii), bf16),
            pltpu.VMEM((chips, rows, tp, 128), bf16),
            pltpu.VMEM((ii, CORES * sub), bf16),
            pltpu.VMEM((ii, sub), bf16),
            pltpu.VMEM((hh, 128), f32),
            pltpu.VMEM((CORES, hh, 128), f32),
            pltpu.VMEM((hh, CORES * sub), f32),
            pltpu.VMEM((hh, CORES * sub), f32),
            pltpu.VMEM((hh, CORES * sub), bf16),
            pltpu.VMEM((ii, sub), f32),
            pltpu.VMEM((ii, sub), f32),
            pltpu.VMEM((ii, sub), f32),
            pltpu.VMEM((ii, CORES * sub), bf16),
            pltpu.VMEM((ii, CORES * sub), bf16),
            pltpu.VMEM((hh, CORES * sub), bf16),
            pltpu.VMEM((2, 8, ii), f32),
            pltpu.VMEM((2, 8, ii), f32),
            pltpu.VMEM((hh, 128), f32),
            pltpu.VMEM((hh, ii), bf16),
            pltpu.VMEM((chips, rows, tp, 128), bf16),
            pltpu.VMEM((rows, hp, ip), bf16),
            pltpu.VMEM((rows, tp, 128), bf16),
            pltpu.VMEM((rows, hp, ip), bf16),
            pltpu.VMEM((rows, tp, 128), bf16),
            pltpu.VMEM((rows, hp, ip), bf16),
            pltpu.VMEM((rows, tp, 128), bf16),
            pltpu.VMEM((rows, hp, ip), bf16),
            pltpu.VMEM((rows, tp, 128), bf16),
            pltpu.VMEM((rows, hp, ip), bf16),
            pltpu.VMEM((rows, tp, 128), bf16),
            pltpu.VMEM((rows, hp, ip), bf16),
            pltpu.VMEM((rows, tp, 128), bf16),
            pltpu.VMEM((hb, ib), f32),
            pltpu.VMEM((hb, ib), f32),
            pltpu.SMEM(bucket.shape, jnp.int32),
            pltpu.VMEM(mod_table.shape[1:], f32),
            pltpu.SemaphoreType.DMA((31 * rows + 36,)),
            pltpu.SemaphoreType.DMA((8,)),
        ],
        compiler_params=pltpu.CompilerParams(
            collective_id=0, has_side_effects=True, vmem_limit_bytes=60 * 1024 * 1024
        ),
    )(bucket, clean, noise, mod_table[0], w_first[0].T, w_second[0])
    out1, out2 = pl.pallas_call(
        hand_over,
        out_shape=(jax.ShapeDtypeStruct((hb, ib), f32), jax.ShapeDtypeStruct((hb, ib), f32)),
        in_specs=[vmem] * 2,
        out_specs=(vmem, vmem),
    )(*(pltpu.with_memory_space_constraint(out, pltpu.VMEM) for out in (out1, out2)))
    return (out1.T[None], out2[None])


def solution(mesh):
    placed = (
        P("row", "col"),
        P("row", "col"),
        P(),
        P(),
        P(None, "row", "col"),
        P(None, "col", "row"),
    )
    return jax.shard_map(
        local_step if mesh.shape["col"] == CORES * SIDE * SIDE else local,
        mesh=mesh,
        in_specs=placed,
        out_specs=(P(None, "row", "col"), P(None, "col", "row")),
        check_vma=False,
    )
```

```python
import math

import jax
import jax.numpy as jnp
from jax import lax
from jax.experimental import pallas as pl
from jax.experimental.pallas import tpu as pltpu
from jax.sharding import PartitionSpec as P

PIX = 256
BUCKETS = 32


MIX_WEIGHT = 0.3
KEEP_COEF = (1.0 - MIX_WEIGHT) / math.sqrt((1.0 - MIX_WEIGHT) ** 2 + MIX_WEIGHT**2)
ADD_COEF = MIX_WEIGHT / math.sqrt((1.0 - MIX_WEIGHT) ** 2 + MIX_WEIGHT**2)
SILU_GAIN = 1.0 / 0.596
CONTRACT_LEAD = (((0,), (0,)), ((), ()))
CONTRACT_TAIL = (((1,), (1,)), ((), ()))


def noise_levels(bucket):
    return jnp.exp(-3.0 + 5.0 * (bucket.astype(jnp.float32) + 0.5) / BUCKETS)


def silu_slope(values):
    sig = jax.nn.sigmoid(values)
    return sig * (1.0 + values * (1.0 - sig))


def bucket_gains(table, picked):
    onehot = (picked[:, None] == jnp.arange(table.shape[0], dtype=jnp.int32)[None, :]).astype(
        jnp.float32
    )
    return jnp.dot(
        onehot, table, precision=lax.Precision.HIGHEST, preferred_element_type=jnp.float32
    )


def local(clean, noise, bucket, mod_table, w_first, w_second):
    rows_size = lax.axis_size("row")
    row_at = lax.axis_index("row")
    col_at = lax.axis_index("col")
    samples = bucket.shape[0]
    own_rows = clean.shape[1]
    weight_first = w_first[0]
    weight_second = w_second[0]
    table = 1.0 + mod_table[0]
    col_first = jnp.sqrt(lax.psum(jnp.sum(weight_first * weight_first, axis=0), "row") + 1.0)
    col_second = jnp.sqrt(lax.psum(jnp.sum(weight_second * weight_second, axis=0), "col") + 1.0)
    normed_first = (weight_first / col_first[None, :]).astype(jnp.bfloat16)
    normed_second = (weight_second / col_second[None, :]).astype(jnp.bfloat16)
    chan_clean, chan_noise = (
        lax.all_to_all(
            clean.astype(jnp.bfloat16), "row", split_axis=1, concat_axis=0, tiled=True
        ).astype(clean.dtype),
        lax.all_to_all(
            noise.astype(jnp.bfloat16), "row", split_axis=1, concat_axis=0, tiled=True
        ).astype(noise.dtype),
    )
    local_clean = chan_clean.T
    local_noise = chan_noise.T
    sub_rows = own_rows // rows_size
    first_row = col_at * own_rows + row_at * sub_rows
    row_sample = (first_row + jnp.arange(sub_rows, dtype=jnp.int32)) // PIX
    row_bucket = jnp.take(bucket, row_sample)
    levels = noise_levels(row_bucket)[:, None]
    spread_root = jnp.sqrt(levels * levels + 0.25)
    state_own = ((local_clean + levels * local_noise) / spread_root).astype(jnp.bfloat16)
    target = local_clean * (2.0 * levels / spread_root) - local_noise * (0.5 / spread_root)
    gains = bucket_gains(table, row_bucket)
    part_first, part_second = (
        lax.all_gather(normed_first, "col", axis=1, tiled=True),
        lax.all_gather(normed_second, "col", axis=0, tiled=True),
    )
    full_first, full_second = (
        lax.all_gather(part_first, "row", axis=0, tiled=True),
        lax.all_gather(part_second, "row", axis=1, tiled=True),
    )
    pre_act = jnp.dot(state_own, full_first, preferred_element_type=jnp.float32)
    hidden = (jax.nn.silu(pre_act) * SILU_GAIN * gains).astype(jnp.bfloat16)
    branch = jnp.dot(hidden, full_second, preferred_element_type=jnp.float32)
    state_new = (KEEP_COEF * state_own.astype(jnp.float32) + ADD_COEF * branch).astype(jnp.bfloat16)
    grad_own = (state_new.astype(jnp.float32) - target) / samples
    dbranch = (ADD_COEF * grad_own).astype(jnp.bfloat16)
    gsecond_full = lax.dot_general(
        hidden, dbranch, CONTRACT_LEAD, preferred_element_type=jnp.float32
    )
    dhidden = lax.dot_general(
        dbranch, full_second, CONTRACT_TAIL, preferred_element_type=jnp.float32
    )
    dpre = (dhidden * gains * silu_slope(pre_act) * SILU_GAIN).astype(jnp.bfloat16)
    gfirst_full = lax.dot_general(
        state_own, dpre, CONTRACT_LEAD, preferred_element_type=jnp.float32
    )
    part_gfirst, part_gsecond = (
        lax.psum_scatter(
            gfirst_full.astype(jnp.bfloat16), "col", scatter_dimension=1, tiled=True
        ).astype(jnp.float32),
        lax.psum_scatter(
            gsecond_full.astype(jnp.bfloat16), "col", scatter_dimension=0, tiled=True
        ).astype(jnp.float32),
    )
    gfirst, gsecond = (
        lax.psum_scatter(
            part_gfirst.astype(jnp.bfloat16), "row", scatter_dimension=0, tiled=True
        ).astype(jnp.float32),
        lax.psum_scatter(
            part_gsecond.astype(jnp.bfloat16), "row", scatter_dimension=1, tiled=True
        ).astype(jnp.float32),
    )
    dot_first = lax.psum(jnp.sum(weight_first * gfirst, axis=0), "row")
    dot_second = lax.psum(jnp.sum(weight_second * gsecond, axis=0), "col")
    grad_first = gfirst / col_first[None, :] - weight_first * (dot_first / col_first**3)[None, :]
    grad_second = (
        gsecond / col_second[None, :] - weight_second * (dot_second / col_second**3)[None, :]
    )
    return (grad_first[None], grad_second[None])


CORES = 2
SIDE = 2
MESH = pl.DeviceIdType.MESH


def round_up(size, unit):
    return -(-size // unit) * unit


def twice(value):
    return jnp.concatenate([value, value], axis=1)


def packing(hb, ib):
    full = ib // 128 * 128
    carried = round_up(ib + 1, 128) - ib
    left = ib - full - carried
    group = round_up(-(-round_up(hb + 2, 16) * max(left, 1) // 128), 16)
    return full, carried, left, group


SINGLE = set(
    [f"s{kind}{m}" for kind in [*"abABCDPxy", "E_C", "F_D"] for m in range(2)]
    + ["s" + kind for kind in "ftgpqnd"] + ["ra0", "rb0", "rP0", "rP1"]
    + ["sz_z00", "sz_z01", "sz_z1"]
)


def split_sum(total):
    high = total.astype(jnp.bfloat16)
    low = (total - high.astype(jnp.float32)).astype(jnp.bfloat16)
    return high, low


def step_kernel(
    hb, ib, samples, names, bucket_h, clean, noise, table_h, w1h, w2h, out1h, out2h,
    cl, no, w1f, w2f, sto, w, wt, st, tg, nrm, gain, pre, slp, hid, brk, brp, brr, dbr, db2, dpre,
    s2, d2, dot1, g, gt, ra0, ra1, sa0, sa1, rb0, rb1, rc0, rc1, pz0, pz1, rz0, rz1, out1, out2,
    bucket, table, sems, local_sems,
):
    ra, sa, rb, rc, pz, rz = (ra0, ra1), (sa0, sa1), (rb0, rb1), (rc0, rc1), (pz0, pz1), (rz0, rz1)
    rows = st.shape[0] // round_up(ib + 1, 128)
    hp, ip = round_up(hb + 2, 16), round_up(ib + 1, 128)
    chips = w.shape[1] // hp
    sub = tg.shape[1]
    hh, ii = chips * hp, rows * ip
    own_rows = cl.shape[1]
    full, carried, left, group = packing(hb, ib)
    tp = wt.shape[2]
    bf16, f32 = jnp.bfloat16, jnp.float32
    z = lax.axis_index("row")
    col = lax.axis_index("col")
    core = lax.rem(col, CORES)
    xy = col // CORES
    x, y = lax.rem(xy, SIDE), xy // SIDE
    xn = y * SIDE + (1 - x)
    yn = (1 - y) * SIDE + x
    dn = (1 - y) * SIDE + (1 - x)
    dev_x = (z, xn * CORES + core)
    dev_y = (z, yn * CORES + core)
    dev_p = (z, xy * CORES + 1 - core)
    up, down = (z + 1, col), (z - 1, col)
    ring = [lax.rem(z + k, rows) for k in range(rows)]
    side = 1 - 2 * (z // (rows // 2))
    steps = [lax.rem(z + side * k + rows, rows) for k in range(1, rows)]
    outer = z // (rows - 1) + (rows - 1 - z) // (rows - 1)
    near = [z] + [outer * steps[k] + (1 - outer) * steps[(k + 2) % 3] for k in range(3)]

    loads = []
    for k, (src, dst) in enumerate([
        (w1h, w1f), (w2h, w2f), (clean, cl), (noise, no), (bucket_h, bucket), (table_h, table)
    ]):
        loads.append(pltpu.make_async_copy(src, dst, local_sems.at[k]))
        loads[-1].start()
    barrier = pltpu.get_barrier_semaphore()
    peers = [dev_x, dev_y, dev_p] + [(ring[k], col) for k in range(1, rows)]
    for peer in peers:
        pl.semaphore_signal(barrier, inc=1, device_id=peer, device_id_type=MESH)

    pending = []

    def sem(kind, at):
        count = 1 if kind in SINGLE else rows
        if kind not in names:
            names[kind] = sum(size for _, size in names.values()), count
        return sems.at[names[kind][0] + (0 if count == 1 else at)]

    def remote(src, dst, kind, at_send, at_recv, dev):
        return pltpu.make_async_remote_copy(
            src_ref=src, dst_ref=dst, send_sem=sem("s" + kind, at_send),
            recv_sem=sem("r" + kind.split("_")[-1], at_recv), device_id=dev, device_id_type=MESH,
        )

    def when(cond, fn):
        if cond is None:
            fn()
        else:
            pl.when(cond)(fn)

    def send(cond, *spec):
        when(cond, lambda: remote(*spec).start())
        if spec[2].startswith("z_") or "s" + spec[2] not in SINGLE:
            pending.append((cond, spec))

    def arrive(cond, dst, kind, at):
        flag = sem("r" + kind, at)
        when(cond, lambda: pltpu.make_async_remote_copy(
            src_ref=dst, dst_ref=dst, send_sem=flag, recv_sem=flag, device_id=dev_p, device_id_type=MESH,
        ).wait_recv())

    def span(start, size, unit):
        return pl.ds(pl.multiple_of(start, unit), size)

    def part_rows(m, p):
        size = hp if m == 0 else tp
        cut = round_up(size // 2, 16) if m == 0 else size // 2 // 16 * 16
        return (0, cut) if p == 0 else (cut, size - cut)

    def wblk(m, xyb, zb, p=None):
        lo, size = (0, hp if m == 0 else tp) if p is None else part_rows(m, p)
        if m == 1:
            return wt.at[xyb, zb, slice(lo, lo + size), :]
        return w.at[0, span(xyb * hp + lo, size, 16), span(zb * ip, ip, 128)]

    tile_lane = lax.broadcasted_iota(jnp.int32, (hp, 128), 1)

    def fold(tail):
        turned = pltpu.roll(tail, 128 - carried, 1)
        folded = jnp.zeros((group, 128), f32)
        for q in range(128 // left):
            piece = turned[q * group : min((q + 1) * group, hp), :]
            piece = jnp.pad(piece, ((0, group - piece.shape[0]), (0, 0)))
            piece = piece if q == 0 else pltpu.roll(piece, left * q, 1)
            folded = jnp.where(tile_lane[:group] // left == q, piece, folded)
        return turned, folded

    def unfold(top, folded):
        pieces = []
        for q in range(128 // left):
            piece = folded if q == 0 else pltpu.roll(folded, 128 - left * q, 1)
            pieces.append(piece[: min(group, hp - q * group), :])
        turned = jnp.where(tile_lane < left, jnp.concatenate(pieces, axis=0), top)
        tail = pltpu.roll(turned, carried, 1)
        return jnp.where(tile_lane < carried + left, tail, 0.0)

    def chan(zb, size=ib):
        return span(zb * ip, size, 16)

    def pix(zb):
        return span(zb * sub, sub, 128)

    mine, other = slice(0, sub), slice(sub, 2 * sub)

    for zb in range(rows):
        pad = slice(zb * ip + ib, (zb + 1) * ip)
        st[pad, :] = jnp.zeros((ip - ib, 2 * sub), bf16)
        tg[pad, :] = jnp.zeros((ip - ib, sub), bf16)

    line = lax.broadcasted_iota(jnp.int32, (hp, ip), 0)
    blocks = []
    for m, whole in enumerate((w1f, w2f)):
        loads[m].wait()
        block = jnp.pad(whole[...], ((0, hp - hb), (0, ip - ib)))
        if m == 0:
            total = jnp.sum(block * block, axis=1, keepdims=True)
            total = jnp.pad(jnp.broadcast_to(total, (hp, 128)), ((0, 256 - hp), (0, 0)))
            total = jnp.pad(total.T[:1, :], ((0, 0), (0, ip - 256)))
        else:
            total = jnp.sum(block * block, axis=0, keepdims=True)
        high, low = split_sum(total)
        block = jnp.where(line == hb, high.astype(f32), block)
        block = jnp.where(line == hb + 1, low.astype(f32), block)
        blocks.append(block)
    turned, folded = fold(blocks[1][:, full:])
    first_tail = jnp.where(tile_lane < ib - full, blocks[0][:, full:], turned)
    w[0, span(xy * hp, hp, 16), span(z * ip, full, 128)] = blocks[0][:, :full].astype(bf16)
    w[0, span(xy * hp, hp, 16), span(z * ip + full, 128, 128)] = first_tail.astype(bf16)
    for k in range(full // 128):
        wt[xy, z, k * hp : (k + 1) * hp, :] = blocks[1][:, k * 128 : (k + 1) * 128].astype(bf16)
    wt[xy, z, full // 128 * hp :, :] = folded.astype(bf16)
    pl.semaphore_wait(barrier, len(peers))

    def along_z(cond, m, zb, go_up, go_down, p=None):
        kind = f"z{m}{'' if p is None else p}"
        block = wblk(m, xy, zb, p)
        if go_up:
            send(both(cond, z + 1 < rows), block, block, kind, z, zb, up)
        if go_down:
            send(both(cond, z > 0), block, block, "z_" + kind, 0, zb, down)

    def gather_wait(kind, region):
        flag = sem(kind, 0)
        copies = pltpu.make_async_remote_copy(
            src_ref=region, dst_ref=region, send_sem=flag, recv_sem=flag, device_id=dev_p, device_id_type=MESH,
        )
        if kind[0] == "s":
            copies.wait_send()
        else:
            copies.wait_recv()

    def both(a, b):
        return b if a is None else jnp.logical_and(a, b)

    def across(cond, m, zb):
        send(cond, wblk(m, xy, zb), wblk(m, xy, zb), f"x{m}", zb, zb, dev_x)
        send(cond, wblk(m, xy, zb), wblk(m, xy, zb), f"y{m}", zb, zb, dev_y)

    def diagonal(cond, m, zb):
        arrive(cond, wblk(m, xn, zb), f"x{m}", zb)
        send(cond, wblk(m, xn, zb, 0), wblk(m, xn, zb, 0), f"a{m}", zb, zb, dev_y)
        arrive(cond, wblk(m, yn, zb), f"y{m}", zb)
        send(cond, wblk(m, yn, zb, 1), wblk(m, yn, zb, 1), f"b{m}", zb, zb, dev_x)

    def sides(d):
        found = []
        for sign in (-1, 1):
            zb = z + sign * side * d
            found.append((jnp.logical_and(zb >= 0, zb < rows), zb))
        return found

    def hop(m, d, p=None, signs=(-1, 1), who=None):
        kind = f"z{m}{'' if p is None else p}"
        for sign in signs:
            zb, zt = z + sign * side * d, z - sign * side
            inside = jnp.logical_and(zb >= 0, zb < rows)
            inside = inside if who is None else jnp.logical_and(inside, who)
            block = wblk(m, xy, zb, p)
            arrive(inside, block, kind, zb)
            if d < rows - 1:
                onward = jnp.logical_and(inside, jnp.logical_and(zt >= 0, zt < rows))
                send(onward, block, block, kind, zb, zb, (zt, col))

    def each_side(fn, m, d):
        if d == 0:
            fn(None, m, z)
        else:
            for cond, zb in sides(d):
                fn(cond, m, zb)

    end = jnp.logical_or(z == 0, z == rows - 1)
    middle = jnp.logical_not(end)
    for p in range(2):
        along_z(None, 0, z, True, True, p)
    along_z(end, 1, z, True, True)
    for m in range(2):
        across(None, m, z)

    loads[2].wait()
    loads[3].wait()
    loads[4].wait()
    loads[5].wait()
    for k in range(rows):
        lanes = slice(k * sub, (k + 1) * sub)
        picked = jnp.full((1, sub), bucket[col * rows + k], jnp.int32)
        level = noise_levels(picked)
        root = jnp.sqrt(level * level + 0.25)
        c, n = cl[:, lanes], no[:, lanes]
        sto[0, :, lanes] = ((c + level * n) / root).astype(bf16)
        sto[1, :, lanes] = (c * (2.0 * level / root) - n * (0.5 / root)).astype(bf16)
    st[chan(z), mine] = sto[0, :, pix(z)]
    tg[chan(z), :] = sto[1, :, pix(z)]

    def state_to_partner(zb):
        send(None, st.at[chan(zb), mine], st.at[chan(zb), other], "f", zb, zb, dev_p)

    def toward(kind, first, d):
        plane, target = (0, st.at[chan(z), mine]) if kind == "t" else (1, tg.at[chan(z), :])
        for direction, steps in ((1, z), (-1, rows - 1 - z)):
            zt = z + direction * d
            send(steps == first, sto.at[plane, :, pix(zt)], target,
                 kind, 0, z, (zt, col))

    def some(fn, wanted, m, d):
        for cond, zb in sides(d):
            fn(jnp.logical_and(cond, wanted), m, zb)

    toward("t", 0, 1)
    state_to_partner(z)
    hop(0, 1, 0)
    hop(0, 1, 1)
    along_z(middle, 1, z, True, True)
    each_side(across, 0, 1)
    each_side(diagonal, 0, 0)
    hop(1, 1, None, (-1,))
    hop(0, 2, 0)
    hop(0, 2, 1)
    each_side(across, 0, 2)
    hop(1, 1, None, (1,))
    toward("t", 1, 1)
    toward("t", 2, 1)
    each_side(diagonal, 0, 1)
    each_side(diagonal, 1, 0)
    hop(0, 3, 0)
    hop(0, 3, 1)
    each_side(across, 0, 3)
    toward("t", 0, 2)
    hop(1, 2, None, (-1, 1), middle)
    toward("t", 1, 2)
    each_side(diagonal, 0, 2)
    each_side(across, 1, 1)
    some(across, middle, 1, 2)
    each_side(diagonal, 0, 3)
    toward("t", 0, 3)
    hop(1, 2, None, (-1, 1), end)
    some(across, end, 1, 2)
    toward("g", 1, 1)
    toward("g", 0, 1)
    stack = []
    for j in range(CORES):
        whose = core if j == 0 else 1 - core
        picked = bucket[(xy * CORES + whose) * rows + z]
        row = 1.0 + table[pl.ds(picked, 1), :]
        for b in range(chips):
            pieces = [row[:, (b * CORES + c) * hb : (b * CORES + c + 1) * hb] for c in range(CORES)]
            piece = jnp.where(core == 0, pieces[0], pieces[1])
            stack.append(jnp.pad(piece, ((0, 0), (0, 256 - hb))))
    def take_state(k):
        zb = near[k]
        arrive(None, st.at[chan(zb), mine], "t", zb)
        state_to_partner(zb)

    take_state(1)
    for p in range(2):
        lo, size = part_rows(0, p)
        gather_wait(f"r{'ab'[p]}0", w.at[0, span(dn * hp + lo, size, 16), :])

    def sums_of(m, b, lanes):
        tail = w[m, (b + 1) * hp - 16 : (b + 1) * hp, lanes].astype(f32)
        at = hb - (hp - 16)
        return tail[at : at + 1, :] + tail[at + 1 : at + 2, :]

    for b in range(chips):
        stack.append(sum(sums_of(0, b, slice(zb * ip, zb * ip + 256)) for zb in range(rows)))
    filler = 128 - len(stack)
    columns = jnp.concatenate(stack + [jnp.zeros((filler, 256), f32)], axis=0).T
    for b in range(chips):
        at = slice(b * hp, (b + 1) * hp)
        for j in range(CORES):
            k = j * chips + b
            gain[j, at, :] = jnp.broadcast_to(columns[:hp, k : k + 1], (hp, 128))
        k = CORES * chips + b
        nrm[at, :] = jnp.broadcast_to(jnp.sqrt(1.0 + columns[:hp, k : k + 1]), (hp, 128))
    half_rows = hh // 2

    def forward(k):
        zb = near[k]
        arrive(None, st.at[chan(zb), other], "f", zb)
        at_in = span(zb * ip, ip, 128)
        for part in range(2):
            at = slice(part * half_rows, (part + 1) * half_rows)
            value = jnp.dot(w[0, at, at_in], st[at_in, :], preferred_element_type=f32)
            if k > 0:
                value = value + pre[at, :]
            if k < rows - 1:
                pre[at, :] = value
                continue
            inverse = twice(1.0 / nrm[at, :])
            for j in range(CORES):
                lanes = slice(j * sub, (j + 1) * sub)
                v = value[:, lanes] * inverse
                sig = jax.nn.sigmoid(v)
                scale = twice(gain[j, at, :]) * SILU_GAIN
                pre[at, lanes] = v
                hid[at, lanes] = (v * sig * scale).astype(bf16)
                slp[at, lanes] = sig * (1.0 + v * (1.0 - sig)) * scale

    def zlanes(zb):
        return span(zb * ip, ip, 128)

    def open_second(i):
        zb = near[i]
        at = zlanes(zb)
        arrive(None, wblk(1, dn, zb, 0), "a1", zb)
        arrive(None, wblk(1, dn, zb, 1), "b1", zb)
        for b in range(chips):
            rows_at = slice(b * hp, (b + 1) * hp)
            for k in range(full // 128):
                w[1, rows_at, span(zb * ip + k * 128, 128, 128)] = wt[b, zb, k * hp : (k + 1) * hp, :]
            tail_at = span(zb * ip + full, 128, 128)
            tail = unfold(w[0, rows_at, tail_at].astype(f32), wt[b, zb, full // 128 * hp :, :].astype(f32))
            w[1, rows_at, tail_at] = tail.astype(bf16)
        total = sum(sums_of(1, b, at) for b in range(chips))
        s2[0, :, at] = jnp.broadcast_to(total, (s2.shape[1], ip))
        send(None, s2.at[0, :, at], s2.at[1, :, at], "n", i, zb, dev_p)

    def branch_part(i):
        zb = near[i]
        at = zlanes(zb)
        partial = lax.dot_general(w[1, :, at], hid[...], CONTRACT_LEAD, preferred_element_type=f32)
        brp[at, :] = partial[:, other]
        send(None, brp.at[at, :], brr.at[at, :], "p", i, zb, dev_p)
        brk[at, :] = partial[:, mine]

    def slope_part(i):
        zb = near[i]
        at = zlanes(zb)
        if i > 0:
            arrive(None, tg.at[chan(zb), :], "g", zb)
        arrive(None, s2.at[1, :, at], "n", zb)
        total = 1.0 + s2[0, :1, at] + s2[1, :1, at]
        norm = jnp.sqrt(jnp.broadcast_to(total, (128, ip)).T)
        inverse = 1.0 / norm
        arrive(None, brr.at[at, :], "p", zb)
        branch = (brk[at, :] + brr[at, :]) * twice(inverse)
        fresh = (KEEP_COEF * st[at, mine].astype(f32) + ADD_COEF * branch).astype(bf16)
        slope = (fresh.astype(f32) - tg[at, :].astype(f32)) / samples
        rounded = (ADD_COEF * slope).astype(bf16)
        dbr[at, mine] = rounded
        send(None, dbr.at[at, mine], dbr.at[at, other], "q", i, zb, dev_p)
        wide_rounded = rounded.astype(f32)
        db2[at, mine] = (wide_rounded * twice(inverse)).astype(bf16)
        product = jnp.sum(branch * wide_rounded, axis=1, keepdims=True) * norm
        d2[0, :, at] = product.T[: d2.shape[1], :]
        send(None, d2.at[0, :, at], d2.at[1, :, at], "d", i, zb, dev_p)

    hidden_line = lax.broadcasted_iota(jnp.int32, (hp, 1), 0)

    def second_part(i):
        zb = near[i]
        at = zlanes(zb)
        if i == 0:
            second = lax.dot_general(hid[:, mine], dbr[at, mine], CONTRACT_TAIL, preferred_element_type=f32)
        arrive(None, dbr.at[at, other], "q", zb)
        arrive(None, d2.at[1, :, at], "d", zb)
        if i == 0:
            second = second + lax.dot_general(
                hid[:, other], dbr[at, other], CONTRACT_TAIL, preferred_element_type=f32
            )
        else:
            second = lax.dot_general(hid[...], dbr[at, :], CONTRACT_TAIL, preferred_element_type=f32)
        dot2 = d2[0, :1, at] + d2[1, :1, at]
        for b in range(chips):
            rows_at = slice(b * hp, (b + 1) * hp)
            part = jnp.where(hidden_line >= hb, dot2, second[rows_at, :])
            for k in range(full // 128):
                gt[b, i, k * hp : (k + 1) * hp, :] = part[:, k * 128 : (k + 1) * 128].astype(bf16)
            turned, folded = fold(part[:, full:])
            gt[b, i, full // 128 * hp :, :] = folded.astype(bf16)
            g[rows_at, span(zb * ip + full, 128, 128)] = turned.astype(bf16)
        total = jnp.broadcast_to(1.0 + s2[0, :1, at] + s2[1, :1, at], (128, ip))
        inverse = 1.0 / jnp.sqrt(total.T)
        db2[at, other] = (dbr[at, other].astype(f32) * twice(inverse)).astype(bf16)

    dot_rows = []

    def backward():
        for part in range(2):
            at = slice(part * half_rows, (part + 1) * half_rows)
            grad = jnp.dot(w[1, at, :], db2[...], preferred_element_type=f32)
            rounded = (grad * slp[at, :]).astype(bf16)
            dpre[at, :] = rounded
            total = jnp.sum(rounded.astype(f32) * pre[at, :], axis=1, keepdims=True)
            dot1[at, :] = total * nrm[at, :]
        for b in range(chips):
            column = jnp.pad(dot1[b * hp : (b + 1) * hp, :], ((0, 256 - hp), (0, 0)))
            dot_rows.append(jnp.pad(column.T[:1, :], ((0, 0), (0, ip - 256))))

    lane = lax.broadcasted_iota(jnp.int32, (1, ip), 1)
    last = near[:0:-1] + [z]
    orders = (last, near)

    def first_part(i):
        zb = last[i]
        at = zlanes(zb)
        first = lax.dot_general(dpre[...], st[at, :], CONTRACT_TAIL, preferred_element_type=f32)
        tail_at = span(zb * ip + full, 128, 128)
        for b in range(chips):
            rows_at = slice(b * hp, (b + 1) * hp)
            part = jnp.where(hidden_line >= hb, dot_rows[b], first[rows_at, :])
            g[rows_at, span(zb * ip, full, 128)] = part[:, :full].astype(bf16)
            turned = g[rows_at, tail_at].astype(f32)
            g[rows_at, tail_at] = jnp.where(tile_lane < ib - full, part[:, full:], turned).astype(bf16)

    def gblk(m, xyb, i, p):
        lo, size = part_rows(m, p)
        if m == 1:
            return gt, (xyb, i, slice(lo, lo + size), slice(None))
        return g, (span(xyb * hp + lo, size, 16), span(last[i] * ip, ip, 128))

    def gref(m, xyb, i, p):
        ref, at = gblk(m, xyb, i, p)
        return ref.at[at]

    def gval(m, xyb, i, p):
        ref, at = gblk(m, xyb, i, p)
        return ref[at].astype(f32)

    def rblk_all(refs, m, lo, size):
        return refs[m].at[:, slice(lo, lo + size), :]

    def rblk(refs, m, i, p):
        lo, size = part_rows(m, p)
        return refs[m].at[i, slice(lo, lo + size), :]

    def legs(p):
        return (yn, dev_y, xn, dev_x) if p == 0 else (xn, dev_x, yn, dev_y)

    def far_leg(m, i):
        for p in range(2):
            nb1, dev1, nb2, dev2 = legs(p)
            send(None, gref(m, dn, i, p), rblk(ra, m, i, p), f"{'AB'[p]}{m}", i, i, dev1)

    def near_leg(m, i):
        for p in range(2):
            nb1, dev1, nb2, dev2 = legs(p)
            send(None, gref(m, nb1, i, p), rblk(rc, m, i, p), f"{'CD'[p]}{m}", i, i, dev1)

    def stage_a(m, i):
        far_leg(m, i)
        near_leg(m, i)

    def stage_b(m, i):
        for p in range(2):
            nb1, dev1, nb2, dev2 = legs(p)
            arrive(None, rblk(ra, m, i, p), f"{'AB'[p]}{m}", i)
            lo, size = part_rows(m, p)
            inside = (i, slice(lo, lo + size))
            sa[m][inside] = (gval(m, nb2, i, p) + ra[m][inside].astype(f32)).astype(bf16)
            send(None, rblk(sa, m, i, p), rblk(rb, m, i, p), f"{'EF'[p]}_{'CD'[p]}{m}", i, i, dev2)

    def stage_c(m, i):
        zb = orders[m][i]
        own = i == (rows - 1 if m == 0 else 0)
        totals = []
        for p in range(2):
            lo, size = part_rows(m, p)
            arrive(None, rb[m].at[0:2, slice(lo, lo + size), :], f"{'CD'[p]}{m}", i)
            inside = (i, slice(lo, lo + size))
            total = gval(m, xy, i, p) + rb[m][inside].astype(f32) + rc[m][inside].astype(f32)
            if own:
                totals.append(total)
            else:
                pz[m][inside] = total.astype(bf16)
                send(None, rblk(pz, m, i, p), rz[m].at[z, slice(lo, lo + size), :], f"P{m}", i, z, (zb, col))
        if own:
            return jnp.concatenate(totals, axis=0)
        return None

    sums = [None, None]
    forward(0)
    forward(1)
    hop(1, 3)
    each_side(across, 1, 3)
    some(diagonal, end, 1, 1)
    take_state(2)
    take_state(3)
    toward("g", 2, 1)
    open_second(0)
    forward(2)
    forward(3)
    toward("g", 1, 2)
    some(diagonal, middle, 1, 1)
    some(diagonal, end, 1, 2)
    branch_part(0)
    toward("g", 0, 2)
    some(diagonal, middle, 1, 2)
    each_side(diagonal, 1, 3)
    open_second(1)
    branch_part(1)
    slope_part(0)
    toward("g", 0, 3)
    slope_part(1)
    second_part(0)
    stage_a(1, 0)
    open_second(2)
    branch_part(2)
    second_part(1)
    stage_a(1, 1)
    open_second(3)
    branch_part(3)
    stage_b(1, 0)
    slope_part(2)
    second_part(2)
    stage_a(1, 2)
    stage_b(1, 1)
    slope_part(3)
    second_part(3)
    stage_a(1, 3)
    backward()
    stage_b(1, 2)
    first_part(0)
    stage_a(0, 0)
    first_part(1)
    stage_b(1, 3)
    stage_a(0, 1)
    stage_c(1, 1)
    first_part(2)
    stage_b(0, 0)
    stage_a(0, 2)
    stage_c(1, 2)
    first_part(3)
    stage_b(0, 1)
    stage_c(1, 3)
    stage_c(0, 0)
    far_leg(0, 3)
    stage_b(0, 2)
    near_leg(0, 3)
    stage_c(0, 1)
    stage_c(0, 2)
    stage_b(0, 3)
    sums[1] = stage_c(1, 0)

    def collect(m, total):
        gather_wait(f"rP{m}", pz[m].at[0 : rows - 1])
        for k in range(1, rows):
            total = total + rz[m][ring[k]].astype(f32)
        return total

    second = collect(1, sums[1])
    norm2 = jnp.sqrt(1.0 + s2[0, :1, zlanes(z)] + s2[1, :1, zlanes(z)])[:, :ib]
    norm1 = nrm[span(xy * hp, hp, 16), :1][:hb]
    first = collect(0, stage_c(0, 3))

    def finish():
        row = jnp.broadcast_to(first[hb : hb + 1, :256], (128, 256))
        dot_first = row.T[:hb, :1]
        out1h[...] = first[:hb, :ib] / norm1 - w1f[...] * (dot_first / (norm1 * norm1 * norm1))
        tail = unfold(first[:, full:], second[full // 128 * hp :, :])
        both_tiles = [second[k * hp : (k + 1) * hp, :] for k in range(full // 128)]
        unpacked = jnp.concatenate(both_tiles + [tail], axis=1)
        dot_second = unpacked[hb : hb + 1, :ib]
        out2h[...] = unpacked[:hb, :ib] / norm2 - w2f[...] * (dot_second / (norm2 * norm2 * norm2))

    finish()
    for cond, spec in pending:
        when(cond, lambda spec=spec: remote(*spec).wait_send())
    for m in range(2):
        for p in range(2):
            lo, size = part_rows(m, p)
            region = rblk_all(rb, m, lo, size)
            for kind in ("ab"[p], "AB"[p], "CD"[p], "EF"[p] + "_" + "CD"[p]):
                gather_wait(f"s{kind}{m}", region)
        gather_wait(f"sP{m}", pz[m].at[0 : rows - 1])
    for kind in ("x", "y"):
        gather_wait(f"s{kind}0", w.at[0, :, 0:ip])
        gather_wait(f"s{kind}1", wt.at[0])
    gather_wait("sf", st.at[0 : rows * ib, mine])
    gather_wait("st", st.at[0 : (rows - 1) * ib, mine])
    gather_wait("sg", st.at[0 : (rows - 1) * ib, mine])
    gather_wait("sp", brp)
    gather_wait("sq", dbr.at[:, mine])
    gather_wait("sn", s2.at[0])
    gather_wait("sd", d2.at[0])
    used = sum(size for _, size in names.values())
    assert used == sems.shape[0], (used, sum(size == 1 for _, size in names.values()))


def hand_over(in1, in2, out1, out2):
    out1[...] = in1[...]
    out2[...] = in2[...]


def local_step(clean, noise, bucket, mod_table, w_first, w_second):
    rows = lax.axis_size("row")
    cols = lax.axis_size("col")
    samples = bucket.shape[0]
    own_rows = clean.shape[1]
    ib, hb = clean.shape[0], w_first.shape[2]
    sub = own_rows // rows
    full, carried, left, group = packing(hb, ib)
    if sub != PIX or rows != 4 or left <= 0 or 128 % left != 0 or hb + 2 > 256:
        return local(clean, noise, bucket, mod_table, w_first, w_second)
    chips = cols // CORES
    hp, ip = round_up(hb + 2, 16), round_up(ib + 1, 128)
    bf16, f32 = jnp.bfloat16, jnp.float32
    hh, ii = chips * hp, rows * ip
    tp = full // 128 * hp + group
    vmem = pl.BlockSpec(memory_space=pltpu.VMEM)
    anywhere = pl.BlockSpec(memory_space=pl.ANY)
    out1, out2 = pl.pallas_call(
        lambda *refs: step_kernel(hb, ib, samples, {}, *refs),
        out_shape=(pltpu.VMEM((hb, ib), f32), pltpu.VMEM((hb, ib), f32)),
        in_specs=[anywhere] * 6,
        out_specs=(vmem, vmem),
        scratch_shapes=[
            pltpu.VMEM((ib, own_rows), f32),
            pltpu.VMEM((ib, own_rows), f32),
            pltpu.VMEM((hb, ib), f32),
            pltpu.VMEM((hb, ib), f32),
            pltpu.VMEM((2, ib, own_rows), bf16),
            pltpu.VMEM((2, hh, ii), bf16),
            pltpu.VMEM((chips, rows, tp, 128), bf16),
            pltpu.VMEM((ii, CORES * sub), bf16),
            pltpu.VMEM((ii, sub), bf16),
            pltpu.VMEM((hh, 128), f32),
            pltpu.VMEM((CORES, hh, 128), f32),
            pltpu.VMEM((hh, CORES * sub), f32),
            pltpu.VMEM((hh, CORES * sub), f32),
            pltpu.VMEM((hh, CORES * sub), bf16),
            pltpu.VMEM((ii, sub), f32),
            pltpu.VMEM((ii, sub), f32),
            pltpu.VMEM((ii, sub), f32),
            pltpu.VMEM((ii, CORES * sub), bf16),
            pltpu.VMEM((ii, CORES * sub), bf16),
            pltpu.VMEM((hh, CORES * sub), bf16),
            pltpu.VMEM((2, 8, ii), f32),
            pltpu.VMEM((2, 8, ii), f32),
            pltpu.VMEM((hh, 128), f32),
            pltpu.VMEM((hh, ii), bf16),
            pltpu.VMEM((chips, rows, tp, 128), bf16),
            pltpu.VMEM((rows, hp, ip), bf16),
            pltpu.VMEM((rows, tp, 128), bf16),
            pltpu.VMEM((rows, hp, ip), bf16),
            pltpu.VMEM((rows, tp, 128), bf16),
            pltpu.VMEM((rows, hp, ip), bf16),
            pltpu.VMEM((rows, tp, 128), bf16),
            pltpu.VMEM((rows, hp, ip), bf16),
            pltpu.VMEM((rows, tp, 128), bf16),
            pltpu.VMEM((rows, hp, ip), bf16),
            pltpu.VMEM((rows, tp, 128), bf16),
            pltpu.VMEM((rows, hp, ip), bf16),
            pltpu.VMEM((rows, tp, 128), bf16),
            pltpu.VMEM((hb, ib), f32),
            pltpu.VMEM((hb, ib), f32),
            pltpu.SMEM(bucket.shape, jnp.int32),
            pltpu.VMEM(mod_table.shape[1:], f32),
            pltpu.SemaphoreType.DMA((27 * rows + 36,)),
            pltpu.SemaphoreType.DMA((8,)),
        ],
        compiler_params=pltpu.CompilerParams(
            collective_id=0, has_side_effects=True, vmem_limit_bytes=60 * 1024 * 1024
        ),
    )(bucket, clean, noise, mod_table[0], w_first[0].T, w_second[0])
    out1, out2 = pl.pallas_call(
        hand_over,
        out_shape=(jax.ShapeDtypeStruct((hb, ib), f32), jax.ShapeDtypeStruct((hb, ib), f32)),
        in_specs=[vmem] * 2,
        out_specs=(vmem, vmem),
    )(*(pltpu.with_memory_space_constraint(out, pltpu.VMEM) for out in (out1, out2)))
    return (out1.T[None], out2[None])


def solution(mesh):
    placed = (
        P("row", "col"),
        P("row", "col"),
        P(),
        P(),
        P(None, "row", "col"),
        P(None, "col", "row"),
    )
    return jax.shard_map(
        local_step if mesh.shape["col"] == CORES * SIDE * SIDE else local,
        mesh=mesh,
        in_specs=placed,
        out_specs=(P(None, "row", "col"), P(None, "col", "row")),
        check_vma=False,
    )
```
